32 devices in a mesh: dp: 4 (over z), row: 2 (over y), col: 4 (over x, core).
Axes of the slice: x: 2, y: 2, z: 4, core: 2. Of those that a mesh axis runs over, the one named last changes fastest.
Arguments:
- block_in: bfloat16 [4, 1024, 2048], P('dp', None, ('row', 'col')), may hold values from -6 to 6
- segment_ids: int32 [4, 1024], P('dp'), may hold values from 0 to 3, never falling along the last dimension, each value on 1 to 512 neighbouring positions
- block_cotangent: bfloat16 [4, 1024, 2048], P('dp', None, ('row', 'col')), may hold values from -6 to 6
- query_weight: bfloat16 [2048, 2048], P('row', 'col'), may hold values from -0.125 to 0.125
- key_weight: bfloat16 [2048, 2048], P('row', 'col'), may hold values from -0.125 to 0.125
- value_weight: bfloat16 [2048, 4096], P('row', 'col'), may hold values from -0.125 to 0.125
- swish_weight: bfloat16 [2048, 4096], P('row', 'col'), may hold values from -0.125 to 0.125
- output_weight: bfloat16 [4096, 2048], P('col', 'row'), may hold values from -0.1875 to 0.1875
- gelu_weight: bfloat16 [2048, 4096], P('row', 'col'), may hold values from -0.125 to 0.125
- up_weight: bfloat16 [2048, 4096], P('row', 'col'), may hold values from -0.125 to 0.125
- down_weight: bfloat16 [4096, 2048], P('col', 'row'), may hold values from -0.1875 to 0.1875
- first_gain: float32 [2048], P(('row', 'col')), may hold values from 0.25 to 1.75
- second_gain: float32 [2048], P(('row', 'col')), may hold values from 0.25 to 1.75
Outputs:
- block_out: bfloat16 [4, 1024, 2048], P('dp', None, ('row', 'col'))
- grad_input: bfloat16 [4, 1024, 2048], P('dp', None, ('row', 'col'))
- grad_query: float32 [2048, 2048], P('row', 'col')
- grad_key: float32 [2048, 2048], P('row', 'col')
- grad_value: float32 [2048, 4096], P('row', 'col')
- grad_swish: float32 [2048, 4096], P('row', 'col')
- grad_output: float32 [4096, 2048], P('col', 'row')
- grad_gelu: float32 [2048, 4096], P('row', 'col')
- grad_up: float32 [2048, 4096], P('row', 'col')
- grad_down: float32 [4096, 2048], P('col', 'row')
- grad_first: float32 [2048], P(('row', 'col'))
- grad_second: float32 [2048], P(('row', 'col'))
The draws below stay inside these ranges and needn't reach their ends.
Inputs may be any that keep to these rules, and one draw needn't show every extreme that they name: `segment_ids`: in each pack the ids never fall; each of the 4 documents has 1 to 512 tokens, and one has exactly 512.
All inputs are finite; a program needn't handle non-finite values.
Results may differ from the reference program's by a relative error of at most 0.017.
Values may be sent and summed in bfloat16 or wider, within the bound.
A program may use at most 192 MiB of HBM per device.

```python
import math
import jax
import jax.numpy as jnp
import numpy as np
from jax import lax

D = 2048
H = 8
KD = 256
VH = 512
FF = 4096
TOK = 1024
SEGS = 4
PACKS = 4


def level_of(stream_key, dims, pieces, low, top_value):
    factor_of = 1.0
    for dim, shards_of in pieces:
        steps = jax.random.uniform(jax.random.fold_in(jax.random.fold_in(stream_key, 6), dim), (shards_of,), jnp.float32, low / len(pieces), top_value / len(pieces))
        factor_of = factor_of * jnp.repeat(jnp.exp(steps), dims[dim] // shards_of).reshape((-1,) + (1,) * (len(dims) - 1 - dim))
    return factor_of


def length_profile(amount, total, bound, skew):
    weights = [(1 << 20) // math.isqrt(standing ** skew) + 1 for standing in range(2, amount + 1)]
    spare, counts = total - bound - (amount - 1), [1] * (amount - 1)
    while spare > 0:
        movable = [i for i in range(amount - 1) if counts[i] < bound]
        pool, left = sum([weights[i] for i in movable]), spare
        for i in movable:
            more = min(bound - counts[i], max(1, left * weights[i] // pool), spare)
            counts[i] = counts[i] + more
            spare = spare - more
    return np.array([bound] + counts)


def uneven_parts(stream_key, number_of, total, most, skew):
    if number_of == 2:
        one = jax.random.randint(stream_key, (), max(1, total - most), min(most, total - 1) + 1)
        return jnp.stack([one, total - one])
    sizes = jnp.asarray(length_profile(number_of, total, most, skew), jnp.int32)
    pairs = (number_of - 1) // 2
    source_of, taker = sizes[1:1 + 2 * pairs:2], sizes[2:2 + 2 * pairs:2]
    room = jnp.minimum(source_of - 1, most - taker)
    passed = jax.random.randint(jax.random.fold_in(stream_key, 1), (pairs,), 0, 1 << 20) % (room + 1)
    sizes = sizes.at[1:1 + 2 * pairs:2].set(source_of - passed).at[2:2 + 2 * pairs:2].set(taker + passed)
    return sizes[jax.random.permutation(jax.random.fold_in(stream_key, 2), number_of)]


def scatter_about(stream_key, shape, width, most, shards=(), kind=jnp.bfloat16):
    gain = level_of(stream_key, shape, shards, -0.22, 0.18) if shards else 1.0
    entries = jax.random.normal(stream_key, shape, jnp.float32) * width * gain
    return jnp.minimum(jnp.maximum(entries, -most), most).astype(kind)


def setup_inputs(seed: int = 0) -> dict:
    splits = jax.random.split(jax.random.key(seed), 14)
    return {
        "block_in": scatter_about(splits[0], (PACKS, TOK, D), 1.0, 6.0, ((0, 4), (2, 8))),
        "segment_ids": jax.vmap(lambda own: jnp.searchsorted(jnp.cumsum(uneven_parts(own, SEGS, TOK, TOK // 2, 0)), jnp.arange(TOK), side="right"))(jax.random.split(splits[1], PACKS)).reshape((PACKS, TOK)).astype(jnp.int32),
        "block_cotangent": scatter_about(splits[2], (PACKS, TOK, D), 1.0, 6.0, ((0, 4), (2, 8))),
        "query_weight": scatter_about(splits[3], (D, H * KD), D ** -0.5, 0.125, ((0, 2), (1, 4))),
        "key_weight": scatter_about(splits[4], (D, H * KD), D ** -0.5, 0.125, ((0, 2), (1, 4))),
        "value_weight": scatter_about(splits[5], (D, H * VH), D ** -0.5, 0.125, ((0, 2), (1, 4))),
        "swish_weight": scatter_about(splits[6], (D, H * VH), D ** -0.5, 0.125, ((0, 2), (1, 4))),
        "output_weight": scatter_about(splits[7], (H * VH, D), (H * VH // 4) ** -0.5, 0.1875, ((0, 4), (1, 2))),
        "gelu_weight": scatter_about(splits[8], (D, FF), D ** -0.5, 0.125, ((0, 2), (1, 4))),
        "up_weight": scatter_about(splits[9], (D, FF), D ** -0.5, 0.125, ((0, 2), (1, 4))),
        "down_weight": scatter_about(splits[10], (FF, D), (FF // 4) ** -0.5, 0.1875, ((0, 4), (1, 2))),
        "first_gain": jnp.clip(1.0 + 0.15 * jax.random.normal(splits[11], (D,), jnp.float32), 0.25, 1.75),
        "second_gain": jnp.clip(1.0 + 0.15 * jax.random.normal(splits[12], (D,), jnp.float32), 0.25, 1.75),
    }


epsilon = 1e-06

@jax.custom_vjp
def low(v):
    return lax.optimization_barrier(v.astype(jnp.bfloat16)).astype(jnp.float32)

@jax.custom_vjp
def low_back(v):
    return v

def low_keep(v):
    return (low(v), None)

def low_pass(kept, grad):
    return (grad,)

def back_keep(v):
    return (v, None)

def back_low(kept, grad):
    return (low(grad),)
low.defvjp(low_keep, low_pass)
low_back.defvjp(back_keep, back_low)

def rotate_half(values):
    half_cols = values.shape[-1] // 2
    return jnp.concatenate([-values[..., half_cols:], values[..., :half_cols]], axis=-1)

def rotary_tables(length, columns):
    half_cols = columns // 2
    frequency = 10000.0 ** (-jnp.arange(half_cols, dtype=jnp.float32) / half_cols)
    angles = jnp.arange(length, dtype=jnp.float32)[:, None] * frequency[None, :]
    cosine_half = jnp.cos(angles)
    sine_half = jnp.sin(angles)
    return (jnp.concatenate([cosine_half, cosine_half], axis=1), jnp.concatenate([sine_half, sine_half], axis=1))

def pack_layer(hidden, segments, params):
    query_weight, key_weight, value_weight, swish_weight, output_weight, gelu_weight, up_weight, down_weight, first_gain, second_gain = params
    highest = lax.Precision.HIGHEST
    tokens = hidden.shape[0]
    scale_one = lax.rsqrt(lax.optimization_barrier(jnp.mean(hidden * hidden, axis=1, keepdims=True)) + epsilon)
    normed_one = low(hidden * scale_one * first_gain)
    query_sum = low_back(jnp.dot(normed_one, query_weight, precision=highest))
    key_sum = low_back(jnp.dot(normed_one, key_weight, precision=highest))
    value_sum = jnp.dot(normed_one, value_weight, precision=highest)
    swish_sum = low_back(jnp.dot(normed_one, swish_weight, precision=highest))
    cosine_table, sine_table = rotary_tables(tokens, KD)
    cosine_table = cosine_table[:, None, :]
    sine_table = sine_table[:, None, :]
    query_heads = query_sum.reshape(tokens, H, KD)
    key_heads = key_sum.reshape(tokens, H, KD)
    query_low = low(query_heads * cosine_table + rotate_half(query_heads) * sine_table)
    key_low = low((key_heads * cosine_table + rotate_half(key_heads) * sine_table) * KD ** (-0.5))
    value_low = low(low_back(value_sum)).reshape(tokens, H, VH)
    positions = jnp.arange(tokens, dtype=jnp.int32)
    distance = positions[:, None] - positions[None, :]
    keep_mask = (distance >= 0) & (segments[:, None] == segments[None, :])
    log_decay = jnp.log(1.0 - 2.0 ** (-5.0 - jnp.arange(H, dtype=jnp.float32)))
    decay = jnp.where(keep_mask[None], jnp.exp(jnp.maximum(distance, 0).astype(jnp.float32)[None] * log_decay[:, None, None]), 0.0)
    scores = low_back(jnp.einsum('qhd,khd->hqk', query_low, key_low, precision=highest))
    weights_low = low(scores * decay)
    retained = low_back(jnp.einsum('hqk,khv->qhv', weights_low, value_low, precision=highest))
    spread = jnp.sqrt(lax.optimization_barrier(jnp.mean(retained * retained, axis=2, keepdims=True)) + epsilon)
    grouped = retained / jnp.maximum(spread, 1.0)
    gated = low(jax.nn.silu(swish_sum) * grouped.reshape(tokens, H * VH))
    attended = low_back(jnp.dot(gated, output_weight, precision=highest))
    middle = hidden + attended
    scale_two = lax.rsqrt(lax.optimization_barrier(jnp.mean(middle * middle, axis=1, keepdims=True)) + epsilon)
    normed_two = low(middle * scale_two * second_gain)
    gelu_sum = low_back(jnp.dot(normed_two, gelu_weight, precision=highest))
    up_sum = low_back(jnp.dot(normed_two, up_weight, precision=highest))
    product = low(jax.nn.gelu(gelu_sum) * up_sum)
    feed = low_back(jnp.dot(product, down_weight, precision=highest))
    return middle + feed

def reference(block_in, segment_ids, block_cotangent, query_weight, key_weight, value_weight, swish_weight, output_weight, gelu_weight, up_weight, down_weight, first_gain, second_gain):
    params = (query_weight.astype(jnp.float32), key_weight.astype(jnp.float32), value_weight.astype(jnp.float32), swish_weight.astype(jnp.float32), output_weight.astype(jnp.float32), gelu_weight.astype(jnp.float32), up_weight.astype(jnp.float32), down_weight.astype(jnp.float32), first_gain.astype(jnp.float32), second_gain.astype(jnp.float32))
    hidden_all = block_in.astype(jnp.float32)
    layer_step = jax.checkpoint(pack_layer)

    def whole_layer(hidden_all, params):
        return lax.map(lambda paired: layer_step(paired[0], paired[1], params), (hidden_all, segment_ids))
    outputs, pullback = jax.vjp(whole_layer, hidden_all, params)
    input_grad, param_grads = pullback(block_cotangent.astype(jnp.float32))
    grad_query, grad_key, grad_value, grad_swish, grad_output, grad_gelu, grad_up, grad_down, grad_first, grad_second = param_grads
    return (outputs.astype(jnp.bfloat16), input_grad.astype(jnp.bfloat16), grad_query, grad_key, grad_value, grad_swish, grad_output, grad_gelu, grad_up, grad_down, grad_first, grad_second)
```

```python
import jax
import jax.numpy as jnp
from jax import lax
from jax.experimental import pallas as pl
from jax.experimental.pallas import tpu as pltpu
from jax.sharding import PartitionSpec as P

KD = 256
QBLK = 512
MESH = pl.DeviceIdType.MESH
VM = pltpu.VMEM
F32 = jnp.float32
BF16 = jnp.bfloat16

epsilon = 1e-06


def rotate_half(values):
    half_cols = values.shape[-1] // 2
    return jnp.concatenate([-values[:, half_cols:], values[:, :half_cols]], axis=-1)


def rotary_tables(length, columns):
    half_cols = columns // 2
    frequency = 10000.0 ** (-jnp.arange(half_cols, dtype=jnp.float32) / half_cols)
    angles = jnp.arange(length, dtype=jnp.float32)[:, None] * frequency[None, :]
    cosine_half = jnp.cos(angles)
    sine_half = jnp.sin(angles)
    return (
        jnp.concatenate([cosine_half, cosine_half], axis=1),
        jnp.concatenate([sine_half, sine_half], axis=1),
    )


def decay_block(segments, row_start, row_count, column_count, log_decay):
    query_pos = row_start + jnp.arange(row_count, dtype=jnp.int32)
    key_pos = jnp.arange(column_count, dtype=jnp.int32)
    distance = query_pos[:, None] - key_pos[None, :]
    same_doc = (
        segments[row_start : row_start + row_count][:, None] == segments[:column_count][None, :]
    )
    keep_mask = (distance >= 0) & same_doc
    return jnp.where(
        keep_mask, jnp.exp(jnp.maximum(distance, 0).astype(jnp.float32) * log_decay), 0.0
    )


def neighbours():
    r, c = lax.axis_index("row"), lax.axis_index("col")
    core = c + 1 - 2 * lax.rem(c, 2)
    across = lax.rem(c + 2, 4)
    return r, c, core, across


def enter():
    r, c, core, across = neighbours()
    barrier = pltpu.get_barrier_semaphore()
    for target in ({"col": core}, {"col": across}, {"row": 1 - r}):
        pl.semaphore_signal(barrier, inc=1, device_id=target, device_id_type=MESH)
    pl.semaphore_wait(barrier, 3)


class Sender:
    def __init__(self, send_sem, recv_sem):
        self.send_sem, self.recv_sem, self.started = send_sem, recv_sem, []

    def __call__(self, src, dst, target):
        slot = len(self.started)
        copy = pltpu.make_async_remote_copy(
            src_ref=src,
            dst_ref=dst,
            send_sem=self.send_sem.at[slot],
            recv_sem=self.recv_sem.at[slot],
            device_id=target,
            device_id_type=MESH,
        )
        copy.start()
        self.started.append(copy)
        return copy


def gather_body(own_ref, out_ref, send, local_sem, side):
    rows, width = own_ref.shape
    half = rows // 2
    r, c, core, across = neighbours()
    to_core, to_x, to_y = {"col": core}, {"col": across}, {"row": 1 - r}

    def view(ref, place, part):
        cols = pl.ds(pl.multiple_of(place * width, width), width)
        if part is None:
            return ref.at[:, cols]
        return ref.at[part * half : (part + 1) * half, cols]

    def own(part):
        return own_ref.at[part * half : (part + 1) * half]

    side_start = side(send, to_core, to_x, to_y)
    x0 = send(own(0), view(out_ref, c, 0), to_x)
    y1 = send(own(1), view(out_ref, 4 + c, 1), to_y)
    x1 = send(own(1), view(out_ref, c, 1), to_x)
    y0 = send(own(0), view(out_ref, 4 + c, 0), to_y)
    late = [send(own_ref, view(out_ref, c, None), to_core)]
    keep = pltpu.make_async_copy(own_ref, view(out_ref, c, None), local_sem)
    keep.start()
    next(side_start)
    x0.wait_recv()
    fy = send(view(out_ref, across, 0), view(out_ref, 4 + across, 0), to_y)
    late.append(send(view(out_ref, across, 0), view(out_ref, across, 0), to_core))
    y1.wait_recv()
    fx = send(view(out_ref, 4 + c, 1), view(out_ref, 4 + c, 1), to_x)
    late.append(send(view(out_ref, 4 + c, 1), view(out_ref, 4 + c, 1), to_core))
    next(side_start)
    x1.wait_recv()
    late.append(send(view(out_ref, across, 1), view(out_ref, across, 1), to_core))
    y0.wait_recv()
    late.append(send(view(out_ref, 4 + c, 0), view(out_ref, 4 + c, 0), to_core))
    next(side_start)
    fy.wait_recv()
    late.append(send(view(out_ref, 4 + across, 0), view(out_ref, 4 + across, 0), to_core))
    fx.wait_recv()
    late.append(send(view(out_ref, 4 + across, 1), view(out_ref, 4 + across, 1), to_core))
    keep.wait()
    for copy in late:
        copy.wait_recv()
    for copy in send.started:
        copy.wait_send()


def no_side(send, to_core, to_x, to_y):
    while True:
        yield


def total_side(vec_ref, total_ref, got):
    def steps(send, to_core, to_x, to_y):
        first = send(vec_ref, got.at[0], to_core)

        def rest():
            first.wait_recv()
            got[3] = vec_ref[...] + got[0]
            second = send(got.at[3], got.at[1], to_x)
            yield
            second.wait_recv()
            got[4] = got[3] + got[1]
            third = send(got.at[4], got.at[2], to_y)
            yield
            third.wait_recv()
            total_ref[...] = got[4] + got[2]
            yield

        return rest()

    return steps


def gather_kernel(own_ref, out_ref, send_sem, recv_sem, local_sem):
    enter()
    gather_body(own_ref, out_ref, Sender(send_sem, recv_sem), local_sem, no_side)


def gather_total_kernel(own_ref, vec_ref, out_ref, total_ref, got, send_sem, recv_sem, local_sem):
    enter()
    gather_body(
        own_ref, out_ref, Sender(send_sem, recv_sem), local_sem, total_side(vec_ref, total_ref, got)
    )


def vmem(count):
    return [pl.BlockSpec(memory_space=VM)] * count


def params(number):
    return pltpu.CompilerParams(
        collective_id=number, has_side_effects=True, vmem_limit_bytes=40 << 20
    )


def plane_gather(own):
    rows, width = own.shape
    return pl.pallas_call(
        gather_kernel,
        out_shape=jax.ShapeDtypeStruct((rows, width * 8), own.dtype),
        in_specs=vmem(1),
        out_specs=vmem(1)[0],
        scratch_shapes=[
            pltpu.SemaphoreType.DMA((13,)),
            pltpu.SemaphoreType.DMA((13,)),
            pltpu.SemaphoreType.DMA(()),
        ],
        compiler_params=params(0),
    )(own)


def plane_gather_total(own, vector):
    rows, width = own.shape
    small = (rows // 128, 128)
    wide, total = pl.pallas_call(
        gather_total_kernel,
        out_shape=(
            jax.ShapeDtypeStruct((rows, width * 8), own.dtype),
            jax.ShapeDtypeStruct(small, F32),
        ),
        in_specs=vmem(2),
        out_specs=tuple(vmem(2)),
        scratch_shapes=[
            pltpu.VMEM((5,) + small, F32),
            pltpu.SemaphoreType.DMA((16,)),
            pltpu.SemaphoreType.DMA((16,)),
            pltpu.SemaphoreType.DMA(()),
        ],
        compiler_params=params(1),
    )(own, vector.reshape(small))
    return wide, total.reshape(rows)


def scatter_body(part_ref, out_ref, stage, from_core, from_x, from_y, send, side):
    rows, width = out_ref.shape
    half = rows // 2
    r, c, core, across = neighbours()
    to_core, to_x, to_y = {"col": core}, {"col": across}, {"row": 1 - r}
    places = (4 + across, across, 4 + c, c)
    other = core - c

    def cols(place):
        return pl.ds(pl.multiple_of(place * width, width), width)

    side_start = side(send, to_core, to_x, to_y)
    first = [
        send(part_ref.at[:, cols(places[i] + other)], from_core.at[i], to_core) for i in range(4)
    ]
    lo, hi = slice(0, half), slice(half, 2 * half)

    def summed(i, part):
        return part_ref[part, cols(places[i])].astype(F32) + from_core[i, part].astype(F32)

    first[0].wait_recv()
    next(side_start)
    stage[0, lo] = summed(0, lo).astype(BF16)
    dx = send(stage.at[0, lo], from_x.at[2], to_x)
    stage[0, hi] = summed(0, hi).astype(BF16)
    dy = send(stage.at[0, hi], from_y.at[2], to_y)
    first[1].wait_recv()
    stage[1, lo] = summed(1, lo).astype(BF16)
    x0 = send(stage.at[1, lo], from_x.at[0], to_x)
    first[2].wait_recv()
    stage[2, hi] = summed(2, hi).astype(BF16)
    y1 = send(stage.at[2, hi], from_y.at[1], to_y)
    next(side_start)
    dy.wait_recv()
    stage[1, hi] = (summed(1, hi) + from_y[2].astype(F32)).astype(BF16)
    x1 = send(stage.at[1, hi], from_x.at[1], to_x)
    dx.wait_recv()
    stage[2, lo] = (summed(2, lo) + from_x[2].astype(F32)).astype(BF16)
    y0 = send(stage.at[2, lo], from_y.at[0], to_y)
    next(side_start)
    first[3].wait_recv()
    x0.wait_recv()
    y1.wait_recv()
    out_ref[lo] = summed(3, lo) + from_x[0].astype(F32)
    out_ref[hi] = summed(3, hi) + from_y[1].astype(F32)
    x1.wait_recv()
    out_ref[hi] = out_ref[hi] + from_x[1].astype(F32)
    y0.wait_recv()
    out_ref[lo] = out_ref[lo] + from_y[0].astype(F32)
    for copy in send.started:
        copy.wait_send()


def scatter_kernel(part_ref, out_ref, stage, from_core, from_x, from_y, send_sem, recv_sem):
    enter()
    scatter_body(
        part_ref, out_ref, stage, from_core, from_x, from_y, Sender(send_sem, recv_sem), no_side
    )


def scatter_total_kernel(
    part_ref, vec_ref, out_ref, total_ref, stage, from_core, from_x, from_y, got, send_sem, recv_sem
):
    enter()
    scatter_body(
        part_ref,
        out_ref,
        stage,
        from_core,
        from_x,
        from_y,
        Sender(send_sem, recv_sem),
        total_side(vec_ref, total_ref, got),
    )


def scatter_scratch(rows, width):
    half = rows // 2
    return [
        pltpu.VMEM((3, rows, width), BF16),
        pltpu.VMEM((4, rows, width), BF16),
        pltpu.VMEM((3, half, width), BF16),
        pltpu.VMEM((3, half, width), BF16),
    ]


def plane_scatter(part):
    rows, wide = part.shape
    width = wide // 8
    return pl.pallas_call(
        scatter_kernel,
        out_shape=jax.ShapeDtypeStruct((rows, width), F32),
        in_specs=vmem(1),
        out_specs=vmem(1)[0],
        scratch_shapes=scatter_scratch(rows, width)
        + [pltpu.SemaphoreType.DMA((10,)), pltpu.SemaphoreType.DMA((10,))],
        compiler_params=params(2),
    )(part)


def plane_scatter_total(part, vector):
    rows, wide = part.shape
    width = wide // 8
    small = (rows // 128, 128)
    out, total = pl.pallas_call(
        scatter_total_kernel,
        out_shape=(jax.ShapeDtypeStruct((rows, width), F32), jax.ShapeDtypeStruct(small, F32)),
        in_specs=vmem(2),
        out_specs=tuple(vmem(2)),
        scratch_shapes=scatter_scratch(rows, width)
        + [
            pltpu.VMEM((5,) + small, F32),
            pltpu.SemaphoreType.DMA((13,)),
            pltpu.SemaphoreType.DMA((13,)),
        ],
        compiler_params=params(3),
    )(part, vector.reshape(small))
    return out, total.reshape(rows)


def swap_rows(values):
    return lax.ppermute(values, "row", [(0, 1), (1, 0)])


def halves_of(values, axis, r):
    size = values.shape[axis] // 2
    mine = lax.dynamic_slice_in_dim(values, r * size, size, axis)
    theirs = lax.dynamic_slice_in_dim(values, (1 - r) * size, size, axis)
    return mine, theirs


def whole_weight(values, axis, r):
    mine, theirs = halves_of(values, axis, r)
    return jnp.concatenate([mine, swap_rows(theirs)], axis=1 - axis)


def sum_packs(grad, axis, r):
    size = grad.shape[1 - axis] // 2
    mine = lax.slice_in_dim(grad, 0, size, axis=1 - axis)
    theirs = swap_rows(lax.slice_in_dim(grad, size, 2 * size, axis=1 - axis))
    mine, theirs = lax.psum((mine, theirs), "dp")
    both = jnp.concatenate([mine, theirs, mine], axis=axis)
    width = mine.shape[axis]
    return lax.dynamic_slice_in_dim(both, r * width, 2 * width, axis).astype(F32)


def matmul(left, right):
    return jnp.dot(left, right, preferred_element_type=jnp.float32)


def weight_grad(inputs, grads):
    return jnp.einsum("tk,tf->kf", inputs, grads, preferred_element_type=jnp.float32).astype(BF16)


def back_product(grads, weights):
    return jnp.einsum("tf,kf->tk", grads, weights, preferred_element_type=jnp.float32)


def group_norm(retained):
    spread = jnp.sqrt(jnp.mean(retained * retained, axis=1, keepdims=True) + epsilon)
    return retained / jnp.maximum(spread, 1.0)


def swish_gate(swish_sum, grouped):
    return jax.nn.silu(swish_sum) * grouped


def gelu_gate(gelu_sum, up_sum):
    return jax.nn.gelu(gelu_sum) * up_sum


def retention(query_low, key_low, value_low, segments, log_decay):
    outputs = []
    for start in range(0, query_low.shape[0], QBLK):
        stop = start + QBLK
        decay = decay_block(segments, start, QBLK, stop, log_decay)
        scores = jnp.einsum(
            "qd,kd->qk", query_low[start:stop], key_low[:stop], preferred_element_type=jnp.float32
        )
        weights_low = (scores * decay).astype(jnp.bfloat16)
        outputs.append(matmul(weights_low, value_low[:stop]))
    return jnp.concatenate(outputs, axis=0)


def retention_back(query_low, key_low, value_low, retained_low, segments, log_decay):
    tokens = query_low.shape[0]
    key_accum = jnp.zeros((tokens, key_low.shape[1]), jnp.float32)
    value_accum = jnp.zeros((tokens, value_low.shape[1]), jnp.float32)
    query_parts = []
    for start in range(0, tokens, QBLK):
        stop = start + QBLK
        decay = decay_block(segments, start, QBLK, stop, log_decay)
        scores = jnp.einsum(
            "qd,kd->qk", query_low[start:stop], key_low[:stop], preferred_element_type=jnp.float32
        )
        weights_low = (scores * decay).astype(jnp.bfloat16)
        weights_grad = jnp.einsum(
            "qv,kv->qk",
            retained_low[start:stop],
            value_low[:stop],
            preferred_element_type=jnp.float32,
        )
        scores_low = (weights_grad * decay).astype(jnp.bfloat16)
        query_parts.append(matmul(scores_low, key_low[:stop]))
        key_accum = key_accum.at[:stop].add(
            jnp.einsum(
                "qk,qd->kd", scores_low, query_low[start:stop], preferred_element_type=jnp.float32
            )
        )
        value_accum = value_accum.at[:stop].add(
            jnp.einsum(
                "qk,qv->kv",
                weights_low,
                retained_low[start:stop],
                preferred_element_type=jnp.float32,
            )
        )
    return jnp.concatenate(query_parts, axis=0), key_accum, value_accum


def shards(
    block_in,
    segment_ids,
    block_cotangent,
    query_weight,
    key_weight,
    value_weight,
    swish_weight,
    output_weight,
    gelu_weight,
    up_weight,
    down_weight,
    first_gain,
    second_gain,
):
    r = lax.axis_index("row")
    hidden = block_in[0].astype(jnp.float32)
    segments = segment_ids[0]
    tokens = hidden.shape[0]
    features = hidden.shape[1] * lax.axis_size("row") * lax.axis_size("col")
    head_index = lax.axis_index("col") * lax.axis_size("row") + r
    log_decay = jnp.log(1.0 - 2.0 ** (-5.0 - head_index.astype(jnp.float32)))
    cosine_table, sine_table = rotary_tables(tokens, KD)

    first_weight = jnp.concatenate(
        [
            whole_weight(query_weight, 1, r),
            whole_weight(key_weight, 1, r),
            whole_weight(value_weight, 1, r),
            whole_weight(swish_weight, 1, r),
        ],
        axis=1,
    )
    out_weight = whole_weight(output_weight, 0, r)
    second_weight = jnp.concatenate(
        [whole_weight(gelu_weight, 1, r), whole_weight(up_weight, 1, r)], axis=1
    )
    last_weight = whole_weight(down_weight, 0, r)
    value_cols = out_weight.shape[0]

    wide_one, square_one = plane_gather_total(
        (hidden * first_gain).astype(BF16), jnp.sum(hidden * hidden, axis=1)
    )
    scale_one = lax.rsqrt(square_one / features + epsilon)[:, None]
    sums_one = matmul(wide_one, first_weight) * scale_one
    query_sum = sums_one[:, :KD]
    key_sum = sums_one[:, KD : 2 * KD]
    value_sum = sums_one[:, 2 * KD : 2 * KD + value_cols]
    swish_sum = sums_one[:, 2 * KD + value_cols :]
    query_low = (query_sum * cosine_table + rotate_half(query_sum) * sine_table).astype(
        jnp.bfloat16
    )
    key_low = ((key_sum * cosine_table + rotate_half(key_sum) * sine_table) * KD ** (-0.5)).astype(
        jnp.bfloat16
    )
    value_low = value_sum.astype(jnp.bfloat16)
    retained = retention(query_low, key_low, value_low, segments, log_decay)
    grouped, group_pull = jax.vjp(group_norm, retained)
    gated_full, swish_pull = jax.vjp(swish_gate, swish_sum, grouped)
    gated = gated_full.astype(jnp.bfloat16)
    middle = hidden + plane_scatter(matmul(gated, out_weight).astype(BF16))

    wide_two, square_two = plane_gather_total(
        (middle * second_gain).astype(BF16), jnp.sum(middle * middle, axis=1)
    )
    scale_two = lax.rsqrt(square_two / features + epsilon)[:, None]
    sums_two = matmul(wide_two, second_weight) * scale_two
    hidden_cols = sums_two.shape[1] // 2
    gelu_sum, up_sum = sums_two[:, :hidden_cols], sums_two[:, hidden_cols:]
    product_full, gelu_pull = jax.vjp(gelu_gate, gelu_sum, up_sum)
    product = product_full.astype(jnp.bfloat16)
    block_out = (middle + plane_scatter(matmul(product, last_weight).astype(BF16))).astype(BF16)

    upstream = block_cotangent[0].astype(jnp.float32)
    wide_feed_grad = plane_gather(block_cotangent[0])
    grad_down = weight_grad(product, wide_feed_grad)
    product_grad = back_product(wide_feed_grad, last_weight)
    gelu_grad, up_grad = gelu_pull(product_grad)
    both_grad = jnp.concatenate([gelu_grad, up_grad], axis=1)
    inner_two = jnp.sum(both_grad * sums_two, axis=1)
    both_low = (both_grad * scale_two).astype(BF16)
    grad_both = weight_grad(wide_two, both_low)
    normed_two_grad, inner_two = plane_scatter_total(
        back_product(both_low, second_weight).astype(BF16), inner_two
    )
    grad_second = jnp.sum(normed_two_grad * middle, axis=0)
    middle_grad = (
        upstream
        + second_gain * normed_two_grad
        - middle * (scale_two**2 * inner_two[:, None] / features)
    )
    wide_attended_grad = plane_gather(middle_grad.astype(BF16))
    grad_output = weight_grad(gated, wide_attended_grad)
    gated_grad = back_product(wide_attended_grad, out_weight)
    swish_grad, grouped_grad = swish_pull(gated_grad)
    (retained_grad,) = group_pull(grouped_grad)
    query_grad, key_grad, value_grad = retention_back(
        query_low, key_low, value_low, retained_grad.astype(BF16), segments, log_decay
    )
    key_grad = key_grad * KD ** (-0.5)
    query_back = query_grad * cosine_table - rotate_half(query_grad) * sine_table
    key_back = key_grad * cosine_table - rotate_half(key_grad) * sine_table
    all_grad = jnp.concatenate([query_back, key_back, value_grad, swish_grad], axis=1)
    inner_one = jnp.sum(all_grad * sums_one, axis=1)
    all_low = (all_grad * scale_one).astype(BF16)
    grad_all = weight_grad(wide_one, all_low)
    normed_one_grad, inner_one = plane_scatter_total(
        back_product(all_low, first_weight).astype(BF16), inner_one
    )
    grad_first = jnp.sum(normed_one_grad * hidden, axis=0)
    grad_input = (
        middle_grad
        + first_gain * normed_one_grad
        - hidden * (scale_one**2 * inner_one[:, None] / features)
    ).astype(BF16)

    grad_first, grad_second = lax.psum((grad_first, grad_second), "dp")
    return (
        block_out[None],
        grad_input[None],
        sum_packs(grad_all[:, :KD], 1, r),
        sum_packs(grad_all[:, KD : 2 * KD], 1, r),
        sum_packs(grad_all[:, 2 * KD : 2 * KD + value_cols], 1, r),
        sum_packs(grad_all[:, 2 * KD + value_cols :], 1, r),
        sum_packs(grad_output, 0, r),
        sum_packs(grad_both[:, :hidden_cols], 1, r),
        sum_packs(grad_both[:, hidden_cols:], 1, r),
        sum_packs(grad_down, 0, r),
        grad_first,
        grad_second,
    )


def solution(mesh):
    activations = P("dp", None, ("row", "col"))
    in_weight, out_weight, gain = P("row", "col"), P("col", "row"), P(("row", "col"))
    return jax.shard_map(
        shards,
        mesh=mesh,
        in_specs=(activations, P("dp", None), activations)
        + (in_weight,) * 4
        + (out_weight, in_weight, in_weight, out_weight, gain, gain),
        out_specs=(activations, activations)
        + (in_weight,) * 4
        + (out_weight, in_weight, in_weight, out_weight, gain, gain),
        check_vma=False,
    )
```

```python
import jax
import jax.numpy as jnp
from jax import lax
from jax.experimental import pallas as pl
from jax.experimental.pallas import tpu as pltpu
from jax.sharding import PartitionSpec as P

KD = 256
QBLK = 512
MESH = pl.DeviceIdType.MESH
VM = pltpu.VMEM
F32 = jnp.float32
BF16 = jnp.bfloat16

epsilon = 1e-06


def rotate_half(values):
    half_cols = values.shape[-1] // 2
    return jnp.concatenate([-values[:, half_cols:], values[:, :half_cols]], axis=-1)


def rotary_tables(length, columns):
    half_cols = columns // 2
    frequency = 10000.0 ** (-jnp.arange(half_cols, dtype=jnp.float32) / half_cols)
    angles = jnp.arange(length, dtype=jnp.float32)[:, None] * frequency[None, :]
    cosine_half = jnp.cos(angles)
    sine_half = jnp.sin(angles)
    return (
        jnp.concatenate([cosine_half, cosine_half], axis=1),
        jnp.concatenate([sine_half, sine_half], axis=1),
    )


def decay_block(segments, row_start, row_count, column_count, log_decay):
    query_pos = row_start + jnp.arange(row_count, dtype=jnp.int32)
    key_pos = jnp.arange(column_count, dtype=jnp.int32)
    distance = query_pos[:, None] - key_pos[None, :]
    same_doc = (
        segments[row_start : row_start + row_count][:, None] == segments[:column_count][None, :]
    )
    keep_mask = (distance >= 0) & same_doc
    return jnp.where(
        keep_mask, jnp.exp(jnp.maximum(distance, 0).astype(jnp.float32) * log_decay), 0.0
    )


def neighbours():
    r, c = lax.axis_index("row"), lax.axis_index("col")
    core = c + 1 - 2 * lax.rem(c, 2)
    across = lax.rem(c + 2, 4)
    return r, c, core, across


def enter():
    r, c, core, across = neighbours()
    barrier = pltpu.get_barrier_semaphore()
    for target in ({"col": core}, {"col": across}, {"row": 1 - r}):
        pl.semaphore_signal(barrier, inc=1, device_id=target, device_id_type=MESH)
    pl.semaphore_wait(barrier, 3)


class Sender:
    def __init__(self, send_sem, recv_sem):
        self.send_sem, self.recv_sem, self.started = send_sem, recv_sem, []

    def __call__(self, src, dst, target):
        slot = len(self.started)
        copy = pltpu.make_async_remote_copy(
            src_ref=src,
            dst_ref=dst,
            send_sem=self.send_sem.at[slot],
            recv_sem=self.recv_sem.at[slot],
            device_id=target,
            device_id_type=MESH,
        )
        copy.start()
        self.started.append(copy)
        return copy


def gather_body(own_ref, out_ref, send, local_sem, side):
    rows, width = own_ref.shape
    half = rows // 2
    r, c, core, across = neighbours()
    to_core, to_x, to_y = {"col": core}, {"col": across}, {"row": 1 - r}

    def view(ref, place, part):
        cols = pl.ds(pl.multiple_of(place * width, width), width)
        if part is None:
            return ref.at[:, cols]
        return ref.at[part * half : (part + 1) * half, cols]

    def own(part):
        return own_ref.at[part * half : (part + 1) * half]

    side_start = side(send, to_core, to_x, to_y)
    x0 = send(own(0), view(out_ref, c, 0), to_x)
    y1 = send(own(1), view(out_ref, 4 + c, 1), to_y)
    x1 = send(own(1), view(out_ref, c, 1), to_x)
    y0 = send(own(0), view(out_ref, 4 + c, 0), to_y)
    late = [send(own_ref, view(out_ref, c, None), to_core)]
    keep = pltpu.make_async_copy(own_ref, view(out_ref, c, None), local_sem)
    keep.start()
    next(side_start)
    x0.wait_recv()
    fy = send(view(out_ref, across, 0), view(out_ref, 4 + across, 0), to_y)
    late.append(send(view(out_ref, across, 0), view(out_ref, across, 0), to_core))
    y1.wait_recv()
    fx = send(view(out_ref, 4 + c, 1), view(out_ref, 4 + c, 1), to_x)
    late.append(send(view(out_ref, 4 + c, 1), view(out_ref, 4 + c, 1), to_core))
    next(side_start)
    x1.wait_recv()
    late.append(send(view(out_ref, across, 1), view(out_ref, across, 1), to_core))
    y0.wait_recv()
    late.append(send(view(out_ref, 4 + c, 0), view(out_ref, 4 + c, 0), to_core))
    next(side_start)
    fy.wait_recv()
    late.append(send(view(out_ref, 4 + across, 0), view(out_ref, 4 + across, 0), to_core))
    fx.wait_recv()
    late.append(send(view(out_ref, 4 + across, 1), view(out_ref, 4 + across, 1), to_core))
    keep.wait()
    for copy in late:
        copy.wait_recv()
    for copy in send.started:
        copy.wait_send()


def no_side(send, to_core, to_x, to_y):
    while True:
        yield


def total_side(vec_ref, total_ref, got):
    def steps(send, to_core, to_x, to_y):
        first = send(vec_ref, got.at[0], to_core)

        def rest():
            first.wait_recv()
            got[3] = vec_ref[...] + got[0]
            second = send(got.at[3], got.at[1], to_x)
            yield
            second.wait_recv()
            got[4] = got[3] + got[1]
            third = send(got.at[4], got.at[2], to_y)
            yield
            third.wait_recv()
            total_ref[...] = got[4] + got[2]
            yield

        return rest()

    return steps


def gather_kernel(own_ref, out_ref, send_sem, recv_sem, local_sem):
    enter()
    gather_body(own_ref, out_ref, Sender(send_sem, recv_sem), local_sem, no_side)


def gather_total_kernel(own_ref, vec_ref, out_ref, total_ref, got, send_sem, recv_sem, local_sem):
    enter()
    gather_body(
        own_ref, out_ref, Sender(send_sem, recv_sem), local_sem, total_side(vec_ref, total_ref, got)
    )


def vmem(count):
    return [pl.BlockSpec(memory_space=VM)] * count


def params(number):
    return pltpu.CompilerParams(
        collective_id=number, has_side_effects=True, vmem_limit_bytes=40 << 20
    )


def plane_gather(own):
    rows, width = own.shape
    return pl.pallas_call(
        gather_kernel,
        out_shape=jax.ShapeDtypeStruct((rows, width * 8), own.dtype),
        in_specs=vmem(1),
        out_specs=vmem(1)[0],
        scratch_shapes=[
            pltpu.SemaphoreType.DMA((13,)),
            pltpu.SemaphoreType.DMA((13,)),
            pltpu.SemaphoreType.DMA(()),
        ],
        compiler_params=params(0),
    )(own)


def plane_gather_total(own, vector):
    rows, width = own.shape
    small = (rows // 128, 128)
    wide, total = pl.pallas_call(
        gather_total_kernel,
        out_shape=(
            jax.ShapeDtypeStruct((rows, width * 8), own.dtype),
            jax.ShapeDtypeStruct(small, F32),
        ),
        in_specs=vmem(2),
        out_specs=tuple(vmem(2)),
        scratch_shapes=[
            pltpu.VMEM((5,) + small, F32),
            pltpu.SemaphoreType.DMA((16,)),
            pltpu.SemaphoreType.DMA((16,)),
            pltpu.SemaphoreType.DMA(()),
        ],
        compiler_params=params(1),
    )(own, vector.reshape(small))
    return wide, total.reshape(rows)


def scatter_body(part_ref, out_ref, stage, from_core, from_x, from_y, send, side):
    rows, width = out_ref.shape
    half = rows // 2
    r, c, core, across = neighbours()
    to_core, to_x, to_y = {"col": core}, {"col": across}, {"row": 1 - r}
    places = (4 + across, across, 4 + c, c)
    other = core - c

    def cols(place):
        return pl.ds(pl.multiple_of(place * width, width), width)

    side_start = side(send, to_core, to_x, to_y)
    first = [
        send(part_ref.at[:, cols(places[i] + other)], from_core.at[i], to_core) for i in range(4)
    ]
    lo, hi = slice(0, half), slice(half, 2 * half)

    def summed(i, part):
        return part_ref[part, cols(places[i])].astype(F32) + from_core[i, part].astype(F32)

    first[0].wait_recv()
    next(side_start)
    stage[0, lo] = summed(0, lo).astype(BF16)
    dx = send(stage.at[0, lo], from_x.at[2], to_x)
    stage[0, hi] = summed(0, hi).astype(BF16)
    dy = send(stage.at[0, hi], from_y.at[2], to_y)
    first[1].wait_recv()
    stage[1, lo] = summed(1, lo).astype(BF16)
    x0 = send(stage.at[1, lo], from_x.at[0], to_x)
    first[2].wait_recv()
    stage[2, hi] = summed(2, hi).astype(BF16)
    y1 = send(stage.at[2, hi], from_y.at[1], to_y)
    next(side_start)
    dy.wait_recv()
    stage[1, hi] = (summed(1, hi) + from_y[2].astype(F32)).astype(BF16)
    x1 = send(stage.at[1, hi], from_x.at[1], to_x)
    dx.wait_recv()
    stage[2, lo] = (summed(2, lo) + from_x[2].astype(F32)).astype(BF16)
    y0 = send(stage.at[2, lo], from_y.at[0], to_y)
    next(side_start)
    first[3].wait_recv()
    x0.wait_recv()
    y1.wait_recv()
    out_ref[lo] = summed(3, lo) + from_x[0].astype(F32)
    out_ref[hi] = summed(3, hi) + from_y[1].astype(F32)
    x1.wait_recv()
    out_ref[hi] = out_ref[hi] + from_x[1].astype(F32)
    y0.wait_recv()
    out_ref[lo] = out_ref[lo] + from_y[0].astype(F32)
    for copy in send.started:
        copy.wait_send()


def scatter_kernel(part_ref, out_ref, stage, from_core, from_x, from_y, send_sem, recv_sem):
    enter()
    scatter_body(
        part_ref, out_ref, stage, from_core, from_x, from_y, Sender(send_sem, recv_sem), no_side
    )


def scatter_total_kernel(
    part_ref, vec_ref, out_ref, total_ref, stage, from_core, from_x, from_y, got, send_sem, recv_sem
):
    enter()
    scatter_body(
        part_ref,
        out_ref,
        stage,
        from_core,
        from_x,
        from_y,
        Sender(send_sem, recv_sem),
        total_side(vec_ref, total_ref, got),
    )


def scatter_scratch(rows, width):
    half = rows // 2
    return [
        pltpu.VMEM((3, rows, width), BF16),
        pltpu.VMEM((4, rows, width), BF16),
        pltpu.VMEM((3, half, width), BF16),
        pltpu.VMEM((3, half, width), BF16),
    ]


def plane_scatter(part):
    rows, wide = part.shape
    width = wide // 8
    return pl.pallas_call(
        scatter_kernel,
        out_shape=jax.ShapeDtypeStruct((rows, width), F32),
        in_specs=vmem(1),
        out_specs=vmem(1)[0],
        scratch_shapes=scatter_scratch(rows, width)
        + [pltpu.SemaphoreType.DMA((10,)), pltpu.SemaphoreType.DMA((10,))],
        compiler_params=params(2),
    )(part)


def plane_scatter_total(part, vector):
    rows, wide = part.shape
    width = wide // 8
    small = (rows // 128, 128)
    out, total = pl.pallas_call(
        scatter_total_kernel,
        out_shape=(jax.ShapeDtypeStruct((rows, width), F32), jax.ShapeDtypeStruct(small, F32)),
        in_specs=vmem(2),
        out_specs=tuple(vmem(2)),
        scratch_shapes=scatter_scratch(rows, width)
        + [
            pltpu.VMEM((5,) + small, F32),
            pltpu.SemaphoreType.DMA((13,)),
            pltpu.SemaphoreType.DMA((13,)),
        ],
        compiler_params=params(3),
    )(part, vector.reshape(small))
    return out, total.reshape(rows)


def swap_rows(values):
    return lax.ppermute(values, "row", [(0, 1), (1, 0)])


def halves_of(values, axis, r):
    size = values.shape[axis] // 2
    mine = lax.dynamic_slice_in_dim(values, r * size, size, axis)
    theirs = lax.dynamic_slice_in_dim(values, (1 - r) * size, size, axis)
    return mine, theirs


def swap_shared(values):
    size = values.shape[0] // lax.axis_size("dp")
    part = lax.dynamic_slice_in_dim(values, lax.axis_index("dp") * size, size, 0)
    return lax.all_gather(swap_rows(part), "dp", axis=0, tiled=True)


PIECE = 128
GROUP = 8
OUT_UNIT = 2
UNITS = 6


def last_kernel(
    wide_one,
    wide_two,
    wide_att,
    gated,
    both_low,
    weight,
    all_low,
    block_in,
    inner_vec,
    second_vec,
    result,
    back,
    inner_out,
    gains,
    part,
    from_edge,
    from_inner,
    big,
    small,
    stream,
    rows_part,
    rows_core,
    rows_x,
    rows_y,
    total_got,
    gain_own,
    gain_got,
    load_sem,
    local_sem,
    plane_send,
    plane_recv,
    gain_send,
    gain_recv,
    *line_sems,
):
    z, r, c = lax.axis_index("dp"), lax.axis_index("row"), lax.axis_index("col")
    _, _, core, across = neighbours()
    barrier = pltpu.get_barrier_semaphore()
    peers = [{"dp": lax.rem(z + k, 4)} for k in (1, 2, 3)]
    peers += [{"row": 1 - r}, {"col": core}, {"col": across}]
    for target in peers:
        pl.semaphore_signal(barrier, inc=1, device_id=target, device_id_type=MESH)
    tokens, width = back.shape
    half = tokens // 2

    def load(slot, src, dst):
        return pltpu.make_async_copy(src, dst, load_sem.at[slot])

    hidden_cols = small.shape[2]
    loads = [
        load(0, wide_two, big.at[0]),
        load(1, both_low.at[:, hidden_cols:], small.at[0]),
        load(2, both_low.at[:, :hidden_cols], small.at[1]),
        load(3, wide_att, big.at[1]),
        load(4, gated, small.at[0]),
        load(5, wide_one, big.at[0]),
    ]
    for i in range(4):
        loads[i].start()

    places = (4 + across, across, 4 + c, c)
    other = core - c

    def weight_load(i):
        place = places[i % 4] + (other if i < 4 else 0)
        rows = pl.ds(pl.multiple_of(place * width, width), width)
        return load(6 + i % 2, weight.at[rows], stream.at[i % 2])

    weight_load(0).start()
    weight_load(1).start()
    pl.semaphore_wait(barrier, len(peers))

    is_edge = (z == 0) | (z == 3)
    is_inner = (z == 1) | (z == 2)
    near = jnp.where(z < 2, 1 - z, 5 - z)
    far = 3 - z
    flip = jnp.where((z == 0) | (z == 1), 1, 0)
    steps = UNITS * GROUP // 2

    def copy(stream_number, slot, src, dst, target):
        send_sem, recv_sem = line_sems[2 * stream_number], line_sems[2 * stream_number + 1]
        return pltpu.make_async_remote_copy(
            src_ref=src,
            dst_ref=dst,
            send_sem=send_sem.at[slot],
            recv_sem=recv_sem.at[slot],
            device_id=target,
            device_id_type=MESH,
        )

    def theirs_pair(q):
        return 2 * q + flip

    def mine_pair(q):
        return 2 * q + 1 - flip

    def final(pair, slot):
        unit, place = pair // GROUP, lax.rem(pair, GROUP)
        is_out = unit == OUT_UNIT
        row = jnp.where(is_out, slot * 512 + (place // 2) * PIECE, place * PIECE)
        col = jnp.where(is_out, lax.rem(place, 2) * 512, slot * 512)
        return result.at[
            unit,
            pl.ds(pl.multiple_of(row, PIECE), PIECE),
            pl.ds(pl.multiple_of(col, 512), 512),
        ]

    def edge_copy(pair):
        return copy(0, pair, part.at[pair], from_edge.at[pair], {"dp": near})

    def inner_copy(q):
        return copy(1, q, part.at[theirs_pair(q)], from_inner.at[q], {"dp": far})

    def row_copy(q):
        pair = mine_pair(q)
        return copy(2, q, part.at[pair, 1 - r], final(pair, r), {"row": 1 - r})

    def row_arrival(q):
        pair = mine_pair(q)
        return copy(2, q, part.at[pair, 1 - r], final(pair, 1 - r), {"row": 1 - r})

    def keep_copy(q):
        pair = mine_pair(q)
        return pltpu.make_async_copy(part.at[pair, r], final(pair, r), local_sem.at[q])

    def own_copy(stream_number, q, pair, target):
        return copy(stream_number, q, part.at[pair, r], final(pair, r), {"dp": target})

    def got_copy(stream_number, q, pair, target):
        return copy(stream_number, q, final(pair, 1 - r), final(pair, 1 - r), {"dp": target})

    def pass_copy(slot, q, pair):
        return copy(7 + slot, q, final(pair, slot), final(pair, slot), {"dp": near})

    def compute(unit, x_ref, g_ref, shift=0):
        def body(j, carry):
            step, k = j // 2, lax.rem(j, 2)
            k = k + flip - 2 * k * flip
            place = 2 * step + k
            pair = unit * GROUP + place
            for slot in range(2):
                if unit == OUT_UNIT:
                    rows, cols = place // 2, lax.rem(place, 2) + 2 * slot
                else:
                    rows, cols = place + GROUP * slot, shift
                x = x_ref[:, pl.ds(pl.multiple_of(rows * PIECE, PIECE), PIECE)]
                g = g_ref[:, pl.ds(pl.multiple_of(cols * 512, 512), 512)]
                value = lax.dot_general(
                    x, g, (((0,), (0,)), ((), ())), preferred_element_type=F32
                )
                part[pair, r if slot == 0 else 1 - r] = value.astype(BF16)

            @pl.when(is_edge)
            def _():
                edge_copy(pair).start()

            return carry

        lax.fori_loop(0, GROUP, body, 0)

    def stage_far(q):
        pair = theirs_pair(q)
        edge_copy(pair).wait_recv()
        part[pair] = (part[pair].astype(F32) + from_edge[pair].astype(F32)).astype(BF16)
        inner_copy(q).start()

    def stage_sum(q):
        pair = mine_pair(q)
        edge_copy(pair).wait_recv()
        inner_copy(q).wait_recv()
        total = part[pair].astype(F32) + from_edge[pair].astype(F32) + from_inner[q].astype(F32)
        part[pair] = total.astype(BF16)
        row_copy(q).start()
        own_copy(3, q, pair, near).start()
        own_copy(4, q, pair, far).start()
        keep_copy(q).start()

    def stage_out(q):
        pair = mine_pair(q)
        row_arrival(q).wait_recv()
        got_copy(5, q, pair, near).start()
        got_copy(6, q, pair, far).start()

    def stage_pass(q):
        pair = theirs_pair(q)
        own_copy(4, q, pair, far).wait_recv()
        got_copy(6, q, pair, far).wait_recv()
        pass_copy(0, q, pair).start()
        pass_copy(1, q, pair).start()

    def step(q):
        for lag, stage in enumerate((stage_far, stage_sum, stage_out, stage_pass)):

            @pl.when((q >= lag) & (q < steps + lag))
            def _():
                stage(q - lag)

    def run_steps(first, last):
        @pl.when(is_inner)
        def _():
            lax.fori_loop(first, last, lambda q, carry: (step(q), carry)[1], 0)

    send = Sender(plane_send, plane_recv)
    to_core, to_x, to_y = {"col": core}, {"col": across}, {"row": 1 - r}
    lo, hi = slice(0, half), slice(half, 2 * half)
    state = {}

    def product(i):
        weight_load(i).wait()

        def body(k, carry):
            rows = pl.ds(pl.multiple_of(k * 256, 256), 256)
            value = lax.dot_general(
                all_low[rows],
                stream[i % 2],
                (((1,), (1,)), ((), ())),
                preferred_element_type=F32,
            )
            rows_part[i, rows] = value.astype(BF16)
            return carry

        lax.fori_loop(0, tokens // 256, body, 0)
        if i < 6:
            weight_load(i + 2).start()

    def summed(i, rows):
        return rows_part[4 + i, rows].astype(F32) + rows_core[i, rows].astype(F32)

    def phase_products():
        state["side"] = total_side(inner_vec, inner_out, total_got)(send, to_core, to_x, to_y)
        state["first"] = []
        for i in range(4):
            product(i)
            state["first"].append(send(rows_part.at[i], rows_core.at[i], to_core))
        next(state["side"])

    def phase_first():
        first = state["first"]
        for i in range(4):
            product(4 + i)
        first[0].wait_recv()
        rows_part[4, lo] = summed(0, lo).astype(BF16)
        state["dx"] = send(rows_part.at[4, lo], rows_x.at[2], to_x)
        rows_part[4, hi] = summed(0, hi).astype(BF16)
        state["dy"] = send(rows_part.at[4, hi], rows_y.at[2], to_y)
        first[1].wait_recv()
        rows_part[5, lo] = summed(1, lo).astype(BF16)
        state["x0"] = send(rows_part.at[5, lo], rows_x.at[0], to_x)
        first[2].wait_recv()
        rows_part[6, hi] = summed(2, hi).astype(BF16)
        state["y1"] = send(rows_part.at[6, hi], rows_y.at[1], to_y)
        next(state["side"])

    def phase_second():
        state["dy"].wait_recv()
        rows_part[5, hi] = (summed(1, hi) + rows_y[2].astype(F32)).astype(BF16)
        state["x1"] = send(rows_part.at[5, hi], rows_x.at[1], to_x)
        state["dx"].wait_recv()
        rows_part[6, lo] = (summed(2, lo) + rows_x[2].astype(F32)).astype(BF16)
        state["y0"] = send(rows_part.at[6, lo], rows_y.at[0], to_y)
        next(state["side"])

    def phase_third():
        state["first"][3].wait_recv()
        state["x0"].wait_recv()
        state["y1"].wait_recv()
        state["x1"].wait_recv()
        state["y0"].wait_recv()
        back[lo] = summed(3, lo) + rows_x[0].astype(F32) + rows_y[0].astype(F32)
        back[hi] = summed(3, hi) + rows_y[1].astype(F32) + rows_x[1].astype(F32)
        first_gain = jnp.sum(back[...] * block_in[...].astype(F32), axis=0, keepdims=True)
        gain_own[0:1] = first_gain
        gain_own[1:2] = second_vec[...]
        for each in gain_copies:
            each.start()

    gain_copies = [
        pltpu.make_async_remote_copy(
            src_ref=gain_own,
            dst_ref=gain_got.at[k - 1],
            send_sem=gain_send.at[k - 1],
            recv_sem=gain_recv.at[k - 1],
            device_id={"dp": lax.rem(z + k, 4)},
            device_id_type=MESH,
        )
        for k in (1, 2, 3)
    ]

    loads[0].wait()
    loads[1].wait()
    compute(0, big.at[0], small.at[0])
    loads[4].start()
    phase_products()
    run_steps(0, 1)
    phase_first()
    run_steps(1, 3)
    loads[2].wait()
    compute(1, big.at[0], small.at[1])
    loads[5].start()
    run_steps(3, 4)
    phase_second()
    run_steps(4, 7)
    loads[3].wait()
    loads[4].wait()
    compute(2, small.at[0], big.at[1])
    phase_third()
    run_steps(7, 11)
    loads[5].wait()
    compute(3, big.at[0], all_low, 0)
    run_steps(11, 15)
    compute(4, big.at[0], all_low, 1)
    run_steps(15, 19)
    compute(5, big.at[0], all_low, 2)
    run_steps(19, steps + 3)

    total = gain_own[...]
    for each in gain_copies:
        each.wait_send()
    for k in range(3):
        gain_copies[k].wait_recv()
        total = total + gain_got[k]
    gains[...] = total
    for each in send.started:
        each.wait_send()

    @pl.when(is_inner)
    def _():
        def body(q, carry):
            pair = mine_pair(q)
            inner_copy(q).wait_send()
            row_copy(q).wait_send()
            own_copy(3, q, pair, near).wait_send()
            own_copy(4, q, pair, far).wait_send()
            got_copy(5, q, pair, near).wait_send()
            got_copy(6, q, pair, far).wait_send()
            keep_copy(q).wait()
            for slot in range(2):
                pass_copy(slot, q, theirs_pair(q)).wait_send()
            return carry

        lax.fori_loop(0, steps, body, 0)

    @pl.when(is_edge)
    def _():
        def body(q, carry):
            edge_copy(theirs_pair(q)).wait_send()
            edge_copy(mine_pair(q)).wait_send()
            own_copy(3, q, mine_pair(q), near).wait_recv()
            got_copy(5, q, mine_pair(q), near).wait_recv()
            for slot in range(2):
                pass_copy(slot, q, theirs_pair(q)).wait_recv()
            return carry

        lax.fori_loop(0, steps, body, 0)


def last_scatter(wide_one, wide_two, wide_att, gated, both_low, weight, all_low, own, inner, second):
    tokens, width = own.shape
    small = (tokens // 128, 128)
    pairs = UNITS * GROUP
    steps = pairs // 2
    shape = (pairs, 2, PIECE, 512)
    half = tokens // 2
    gain_shape = (8, width)
    scratch = [
        pltpu.VMEM(shape, BF16),
        pltpu.VMEM(shape, BF16),
        pltpu.VMEM((steps,) + shape[1:], BF16),
        pltpu.VMEM((2,) + wide_one.shape, BF16),
        pltpu.VMEM((2,) + gated.shape, BF16),
        pltpu.VMEM((2, width, weight.shape[1]), BF16),
        pltpu.VMEM((8, tokens, width), BF16),
        pltpu.VMEM((4, tokens, width), BF16),
        pltpu.VMEM((3, half, width), BF16),
        pltpu.VMEM((3, half, width), BF16),
        pltpu.VMEM((5,) + small, F32),
        pltpu.VMEM(gain_shape, F32),
        pltpu.VMEM((3,) + gain_shape, F32),
        pltpu.SemaphoreType.DMA((8,)),
        pltpu.SemaphoreType.DMA((steps,)),
        pltpu.SemaphoreType.DMA((13,)),
        pltpu.SemaphoreType.DMA((13,)),
        pltpu.SemaphoreType.DMA((3,)),
        pltpu.SemaphoreType.DMA((3,)),
    ]
    for size in (pairs,) + (steps,) * 8:
        scratch += [pltpu.SemaphoreType.DMA((size,))] * 2
    anywhere = pl.BlockSpec(memory_space=pl.ANY)
    result, back, total, gains = pl.pallas_call(
        last_kernel,
        out_shape=(
            jax.ShapeDtypeStruct((UNITS, 1024, 1024), BF16),
            jax.ShapeDtypeStruct((tokens, width), F32),
            jax.ShapeDtypeStruct(small, F32),
            jax.ShapeDtypeStruct(gain_shape, F32),
        ),
        in_specs=[anywhere] * 6 + vmem(4),
        out_specs=(anywhere,) + tuple(vmem(3)),
        scratch_shapes=scratch,
        compiler_params=pltpu.CompilerParams(
            collective_id=4, has_side_effects=True, vmem_limit_bytes=62 << 20
        ),
        name="last_scatter",
    )(
        wide_one,
        wide_two,
        wide_att,
        gated,
        both_low,
        weight,
        all_low,
        own,
        inner.reshape(small),
        second.reshape(1, width),
    )
    return result, back, total.reshape(tokens), gains[0], gains[1]


def place_halves(mine, theirs, axis, r):
    both = jnp.concatenate([mine, theirs, mine], axis=axis)
    width = mine.shape[axis]
    return lax.dynamic_slice_in_dim(both, r * width, 2 * width, axis).astype(F32)


def sum_packs(grads):
    r = lax.axis_index("row")
    totals = lax.psum(tuple(grad for grad, axis in grads), "dp")
    placed = []
    for total, (grad, axis) in zip(totals, grads):
        size = total.shape[1 - axis] // 2
        mine = lax.slice_in_dim(total, 0, size, axis=1 - axis)
        theirs = swap_rows(lax.slice_in_dim(total, size, 2 * size, axis=1 - axis))
        placed.append(place_halves(mine, theirs, axis, r))
    return placed


def matmul(left, right):
    return jnp.dot(left, right, preferred_element_type=jnp.float32)


def weight_grad(inputs, grads):
    return jnp.einsum("tk,tf->kf", inputs, grads, preferred_element_type=jnp.float32).astype(BF16)


def back_product(grads, weights):
    return jnp.einsum("tf,kf->tk", grads, weights, preferred_element_type=jnp.float32)


def group_norm(retained):
    spread = jnp.sqrt(jnp.mean(retained * retained, axis=1, keepdims=True) + epsilon)
    return retained / jnp.maximum(spread, 1.0)


def swish_gate(swish_sum, grouped):
    return jax.nn.silu(swish_sum) * grouped


def gelu_gate(gelu_sum, up_sum):
    return jax.nn.gelu(gelu_sum) * up_sum


def retention(query_low, key_low, value_low, segments, log_decay):
    outputs = []
    for start in range(0, query_low.shape[0], QBLK):
        stop = start + QBLK
        decay = decay_block(segments, start, QBLK, stop, log_decay)
        scores = jnp.einsum(
            "qd,kd->qk", query_low[start:stop], key_low[:stop], preferred_element_type=jnp.float32
        )
        weights_low = (scores * decay).astype(jnp.bfloat16)
        outputs.append(matmul(weights_low, value_low[:stop]))
    return jnp.concatenate(outputs, axis=0)


def retention_back(query_low, key_low, value_low, retained_low, segments, log_decay):
    tokens = query_low.shape[0]
    key_accum = jnp.zeros((tokens, key_low.shape[1]), jnp.float32)
    value_accum = jnp.zeros((tokens, value_low.shape[1]), jnp.float32)
    query_parts = []
    for start in range(0, tokens, QBLK):
        stop = start + QBLK
        decay = decay_block(segments, start, QBLK, stop, log_decay)
        scores = jnp.einsum(
            "qd,kd->qk", query_low[start:stop], key_low[:stop], preferred_element_type=jnp.float32
        )
        weights_low = (scores * decay).astype(jnp.bfloat16)
        weights_grad = jnp.einsum(
            "qv,kv->qk",
            retained_low[start:stop],
            value_low[:stop],
            preferred_element_type=jnp.float32,
        )
        scores_low = (weights_grad * decay).astype(jnp.bfloat16)
        query_parts.append(matmul(scores_low, key_low[:stop]))
        key_accum = key_accum.at[:stop].add(
            jnp.einsum(
                "qk,qd->kd", scores_low, query_low[start:stop], preferred_element_type=jnp.float32
            )
        )
        value_accum = value_accum.at[:stop].add(
            jnp.einsum(
                "qk,qv->kv",
                weights_low,
                retained_low[start:stop],
                preferred_element_type=jnp.float32,
            )
        )
    return jnp.concatenate(query_parts, axis=0), key_accum, value_accum


def shards(
    block_in,
    segment_ids,
    block_cotangent,
    query_weight,
    key_weight,
    value_weight,
    swish_weight,
    output_weight,
    gelu_weight,
    up_weight,
    down_weight,
    first_gain,
    second_gain,
):
    r = lax.axis_index("row")
    hidden = block_in[0].astype(jnp.float32)
    segments = segment_ids[0]
    tokens = hidden.shape[0]
    features = hidden.shape[1] * lax.axis_size("row") * lax.axis_size("col")
    head_index = lax.axis_index("col") * lax.axis_size("row") + r
    log_decay = jnp.log(1.0 - 2.0 ** (-5.0 - head_index.astype(jnp.float32)))
    cosine_table, sine_table = rotary_tables(tokens, KD)

    heads = [halves_of(w, 1, r) for w in (query_weight, key_weight, value_weight, swish_weight)]
    first_mine = jnp.concatenate([mine for mine, _ in heads], axis=1)
    first_theirs = jnp.concatenate(
        [swap_shared(jnp.concatenate([theirs for _, theirs in heads[:3]], axis=1)), swap_rows(heads[3][1])],
        axis=1,
    )
    units = [halves_of(gelu_weight, 1, r), halves_of(up_weight, 1, r)]
    ends = [halves_of(output_weight, 0, r), halves_of(down_weight, 0, r)]
    value_cols = ends[0][0].shape[0]
    hidden_cols = ends[1][0].shape[0]
    rest = swap_shared(
        jnp.concatenate(
            [units[0][1], units[1][1], jnp.concatenate([ends[0][1], ends[1][1]], axis=0)], axis=1
        )
    )
    second_mine = jnp.concatenate([units[0][0], units[1][0]], axis=1)
    second_theirs = rest[:, : 2 * hidden_cols]
    out_weight = jnp.concatenate([ends[0][0], rest[:value_cols, 2 * hidden_cols :]], axis=1)
    last_weight = jnp.concatenate([ends[1][0], rest[value_cols:, 2 * hidden_cols :]], axis=1)
    first_weight = jnp.concatenate([first_mine, first_theirs], axis=0)
    second_weight = jnp.concatenate([second_mine, second_theirs], axis=0)

    wide_one, square_one = plane_gather_total(
        (hidden * first_gain).astype(BF16), jnp.sum(hidden * hidden, axis=1)
    )
    scale_one = lax.rsqrt(square_one / features + epsilon)[:, None]
    split = first_mine.shape[0]
    sums_one = (
        matmul(wide_one[:, :split], first_mine) + matmul(wide_one[:, split:], first_theirs)
    ) * scale_one
    query_sum = sums_one[:, :KD]
    key_sum = sums_one[:, KD : 2 * KD]
    value_sum = sums_one[:, 2 * KD : 2 * KD + value_cols]
    swish_sum = sums_one[:, 2 * KD + value_cols :]
    query_low = (query_sum * cosine_table + rotate_half(query_sum) * sine_table).astype(
        jnp.bfloat16
    )
    key_low = ((key_sum * cosine_table + rotate_half(key_sum) * sine_table) * KD ** (-0.5)).astype(
        jnp.bfloat16
    )
    value_low = value_sum.astype(jnp.bfloat16)
    retained = retention(query_low, key_low, value_low, segments, log_decay)
    grouped, group_pull = jax.vjp(group_norm, retained)
    gated_full, swish_pull = jax.vjp(swish_gate, swish_sum, grouped)
    gated = gated_full.astype(jnp.bfloat16)
    middle = hidden + plane_scatter(matmul(gated, out_weight).astype(BF16))

    wide_two, square_two = plane_gather_total(
        (middle * second_gain).astype(BF16), jnp.sum(middle * middle, axis=1)
    )
    scale_two = lax.rsqrt(square_two / features + epsilon)[:, None]
    sums_two = matmul(wide_two, second_weight) * scale_two
    gelu_sum, up_sum = sums_two[:, :hidden_cols], sums_two[:, hidden_cols:]
    product_full, gelu_pull = jax.vjp(gelu_gate, gelu_sum, up_sum)
    product = product_full.astype(jnp.bfloat16)
    block_out = (middle + plane_scatter(matmul(product, last_weight).astype(BF16))).astype(BF16)

    upstream = block_cotangent[0].astype(jnp.float32)
    wide_feed_grad = plane_gather(block_cotangent[0])
    product_grad = back_product(wide_feed_grad, last_weight)
    gelu_grad, up_grad = gelu_pull(product_grad)
    both_grad = jnp.concatenate([gelu_grad, up_grad], axis=1)
    inner_two = jnp.sum(both_grad * sums_two, axis=1)
    both_low = (both_grad * scale_two).astype(BF16)
    normed_two_grad, inner_two = plane_scatter_total(
        back_product(both_low, second_weight).astype(BF16), inner_two
    )
    middle_grad = (
        upstream
        + second_gain * normed_two_grad
        - middle * (scale_two**2 * inner_two[:, None] / features)
    )
    wide_attended_grad = plane_gather(middle_grad.astype(BF16))
    gated_grad = back_product(wide_attended_grad, out_weight)
    swish_grad, grouped_grad = swish_pull(gated_grad)
    (retained_grad,) = group_pull(grouped_grad)
    query_grad, key_grad, value_grad = retention_back(
        query_low, key_low, value_low, retained_grad.astype(BF16), segments, log_decay
    )
    key_grad = key_grad * KD ** (-0.5)
    query_back = query_grad * cosine_table - rotate_half(query_grad) * sine_table
    key_back = key_grad * cosine_table - rotate_half(key_grad) * sine_table
    all_grad = jnp.concatenate([query_back, key_back, value_grad, swish_grad], axis=1)
    inner_one = jnp.sum(all_grad * sums_one, axis=1)
    all_low = (all_grad * scale_one).astype(BF16)
    own_second = jnp.sum(normed_two_grad * middle, axis=0)
    if lax.axis_size("dp") == 4:
        (grad_down,) = sum_packs(((weight_grad(product, wide_feed_grad), 0),))
        result, normed_one_grad, inner_one, grad_first, grad_second = last_scatter(
            wide_one,
            wide_two,
            wide_attended_grad,
            gated,
            both_low,
            first_weight,
            all_low,
            block_in[0],
            inner_one,
            own_second,
        )
        grad_up, grad_gelu, grad_output = [result[i].astype(F32) for i in range(3)]
        starts = (0, 2 * KD)
        grad_query, grad_key = [
            jnp.concatenate(
                [result[3, :, side + shift : side + shift + KD] for side in starts], axis=1
            ).astype(F32)
            for shift in (0, KD)
        ]
        grad_value, grad_swish = result[4].astype(F32), result[5].astype(F32)
    else:
        normed_one_grad, inner_one = plane_scatter_total(
            back_product(all_low, first_weight).astype(BF16), inner_one
        )
        grad_first, grad_second = lax.psum(
            (jnp.sum(normed_one_grad * hidden, axis=0), own_second), "dp"
        )
        grad_all = weight_grad(wide_one, all_low)
        (
            grad_query,
            grad_key,
            grad_value,
            grad_swish,
            grad_output,
            grad_gelu,
            grad_up,
            grad_down,
        ) = sum_packs(
            (
                (grad_all[:, :KD], 1),
                (grad_all[:, KD : 2 * KD], 1),
                (grad_all[:, 2 * KD : 2 * KD + value_cols], 1),
                (grad_all[:, 2 * KD + value_cols :], 1),
                (weight_grad(gated, wide_attended_grad), 0),
                (weight_grad(wide_two, both_low[:, :hidden_cols]), 1),
                (weight_grad(wide_two, both_low[:, hidden_cols:]), 1),
                (weight_grad(product, wide_feed_grad), 0),
            )
        )
    grad_input = (
        middle_grad
        + first_gain * normed_one_grad
        - hidden * (scale_one**2 * inner_one[:, None] / features)
    ).astype(BF16)

    return (
        block_out[None],
        grad_input[None],
        grad_query,
        grad_key,
        grad_value,
        grad_swish,
        grad_output,
        grad_gelu,
        grad_up,
        grad_down,
        grad_first,
        grad_second,
    )


def solution(mesh):
    activations = P("dp", None, ("row", "col"))
    in_weight, out_weight, gain = P("row", "col"), P("col", "row"), P(("row", "col"))
    return jax.shard_map(
        shards,
        mesh=mesh,
        in_specs=(activations, P("dp", None), activations)
        + (in_weight,) * 4
        + (out_weight, in_weight, in_weight, out_weight, gain, gain),
        out_specs=(activations, activations)
        + (in_weight,) * 4
        + (out_weight, in_weight, in_weight, out_weight, gain, gain),
        check_vma=False,
    )
```

```python
import jax
import jax.numpy as jnp
from jax import lax
from jax.experimental import pallas as pl
from jax.experimental.pallas import tpu as pltpu
from jax.sharding import PartitionSpec as P

KD = 256
QBLK = 512
MESH = pl.DeviceIdType.MESH
VM = pltpu.VMEM
F32 = jnp.float32
BF16 = jnp.bfloat16

epsilon = 1e-06


def rotate_half(values):
    half_cols = values.shape[-1] // 2
    return jnp.concatenate([-values[:, half_cols:], values[:, :half_cols]], axis=-1)


def rotary_tables(length, columns):
    half_cols = columns // 2
    frequency = 10000.0 ** (-jnp.arange(half_cols, dtype=jnp.float32) / half_cols)
    angles = jnp.arange(length, dtype=jnp.float32)[:, None] * frequency[None, :]
    cosine_half = jnp.cos(angles)
    sine_half = jnp.sin(angles)
    return (
        jnp.concatenate([cosine_half, cosine_half], axis=1),
        jnp.concatenate([sine_half, sine_half], axis=1),
    )


def decay_block(segments, row_start, row_count, column_count, log_decay):
    query_pos = row_start + jnp.arange(row_count, dtype=jnp.int32)
    key_pos = jnp.arange(column_count, dtype=jnp.int32)
    distance = query_pos[:, None] - key_pos[None, :]
    same_doc = (
        segments[row_start : row_start + row_count][:, None] == segments[:column_count][None, :]
    )
    keep_mask = (distance >= 0) & same_doc
    return jnp.where(
        keep_mask, jnp.exp(jnp.maximum(distance, 0).astype(jnp.float32) * log_decay), 0.0
    )


def neighbours():
    r, c = lax.axis_index("row"), lax.axis_index("col")
    core = c + 1 - 2 * lax.rem(c, 2)
    across = lax.rem(c + 2, 4)
    return r, c, core, across


def plane_peers():
    r, c, core, across = neighbours()
    return [{"col": core}, {"col": across}, {"row": 1 - r}]


def line_peers():
    z = lax.axis_index("dp")
    return [{"dp": lax.rem(z + k, 4)} for k in (1, 2, 3)]


def enter(peers):
    barrier = pltpu.get_barrier_semaphore()
    for target in peers:
        pl.semaphore_signal(barrier, inc=1, device_id=target, device_id_type=MESH)
    pl.semaphore_wait(barrier, len(peers))


class Sender:
    def __init__(self, send_sem, recv_sem):
        self.send_sem, self.recv_sem, self.started, self.slots = send_sem, recv_sem, [], 0

    def make(self, src, dst, target):
        slot = self.slots
        self.slots += 1
        return pltpu.make_async_remote_copy(
            src_ref=src,
            dst_ref=dst,
            send_sem=self.send_sem.at[slot],
            recv_sem=self.recv_sem.at[slot],
            device_id=target,
            device_id_type=MESH,
        )

    def __call__(self, src, dst, target):
        copy = self.make(src, dst, target)
        copy.start()
        self.started.append(copy)
        return copy

    def finish(self):
        for copy in self.started:
            copy.wait_send()
        self.started = []


def run(*generators):
    waiting = list(generators)
    while waiting:
        waiting = [each for each in waiting if next(each, "end") != "end"]


def gather_steps(own_ref, out_ref, send, local_sem):
    rows, width = own_ref.shape
    half = rows // 2
    r, c, core, across = neighbours()
    to_core, to_x, to_y = plane_peers()

    def view(place, part):
        cols = pl.ds(pl.multiple_of(place * width, width), width)
        if part is None:
            return out_ref.at[:, cols]
        return out_ref.at[part * half : (part + 1) * half, cols]

    def own(part):
        return own_ref.at[part * half : (part + 1) * half]

    def forward(place, part, target, there):
        return send(view(place, part), view(there, part), target)

    y1 = send(own(1), view(4 + c, 1), to_y)
    x0 = send(own(0), view(c, 0), to_x)
    y0 = send(own(0), view(4 + c, 0), to_y)
    x1 = send(own(1), view(c, 1), to_x)
    late = [send(own_ref, view(c, None), to_core)]
    keep = pltpu.make_async_copy(own_ref, view(c, None), local_sem)
    keep.start()
    yield
    x0.wait_recv()
    late.append(forward(across, 0, to_core, across))
    diag0 = forward(across, 0, to_y, 4 + across)
    yield
    y1.wait_recv()
    diag1 = forward(4 + c, 1, to_x, 4 + c)
    late.append(forward(4 + c, 1, to_core, 4 + c))
    yield
    x1.wait_recv()
    late.append(forward(across, 1, to_core, across))
    y0.wait_recv()
    late.append(forward(4 + c, 0, to_core, 4 + c))
    yield
    diag0.wait_recv()
    late.append(forward(4 + across, 0, to_core, 4 + across))
    yield
    diag1.wait_recv()
    late.append(forward(4 + across, 1, to_core, 4 + across))
    keep.wait()
    for copy in late:
        copy.wait_recv()


GATHERS = 13


def gather_timed(own_ref, out_ref, send, local_sem, rounds, by_x):
    rows, width = own_ref.shape
    half = rows // 2
    r, c, core, across = neighbours()
    to_core, to_x, to_y = plane_peers()
    now = 0

    def view(place, part):
        cols = pl.ds(pl.multiple_of(place * width, width), width)
        if part is None:
            return out_ref.at[:, cols]
        return out_ref.at[part * half : (part + 1) * half, cols]

    def forward(place, part, target, there):
        return send(view(place, part), view(there, part), target)

    keep = pltpu.make_async_copy(own_ref, view(c, None), local_sem)
    late, diagonal = [], []
    first = over = None
    stages = sorted(rounds.items(), key=lambda item: item[1])
    for name, at in stages:
        while now < at:
            now += 1
            yield
        if name == "x":
            keep.start()
            first = send(own_ref, view(c, None), to_x)
            late.append(send(own_ref, view(c, None), to_core))
        elif name == "y":
            over = send(own_ref, view(4 + c, None), to_y)
        elif name == "x_here":
            first.wait_recv()
            late.append(forward(across, None, to_core, across))
            if not by_x:
                diagonal.append(forward(across, 0, to_y, 4 + across))
        elif name == "y_here":
            over.wait_recv()
            late.append(forward(4 + c, None, to_core, 4 + c))
            if by_x:
                diagonal.append(forward(4 + c, None, to_x, 4 + c))
            else:
                diagonal.append(forward(4 + c, 1, to_x, 4 + c))
        elif name == "diagonal":
            for copy in diagonal:
                copy.wait_recv()
            late.append(forward(4 + across, None, to_core, 4 + across))
    keep.wait()
    yield
    for copy in late:
        copy.wait_recv()


def total_steps(vec_ref, total_ref, got, send):
    to_core, to_x, to_y = plane_peers()
    first = send(vec_ref, got.at[0], to_core)
    yield
    first.wait_recv()
    got[3] = vec_ref[...] + got[0]
    second = send(got.at[3], got.at[1], to_x)
    yield
    second.wait_recv()
    got[4] = got[3] + got[1]
    third = send(got.at[4], got.at[2], to_y)
    yield
    third.wait_recv()
    total_ref[...] = got[4] + got[2]


class Weight:
    def __init__(self, source, target, kind, shift, part, parts):
        self.source, self.target, self.kind, self.shift = source, target, kind, shift
        self.part, self.parts, self.shape = part, parts, source.shape

    def span(self, base, length, quarter):
        if quarter is None:
            size = length // self.parts
            return pl.ds(pl.multiple_of(base + self.part * size, size), size)
        size = length // (4 * self.parts)
        return pl.ds(pl.multiple_of(base + (quarter * self.parts + self.part) * size, size), size)

    def held(self, side, quarter):
        rows, cols = self.shape
        if self.kind == "in":
            width = cols // 2
            columns = pl.ds(pl.multiple_of(side * width, width), width)
            return self.source.at[self.span(0, rows, quarter), columns]
        return self.source.at[self.span(side * (rows // 2), rows // 2, quarter), :]

    def whole(self, other, quarter):
        rows, cols = self.shape
        if self.kind == "in":
            return self.target.at[
                self.span(other * rows, rows, quarter), self.shift : self.shift + cols // 2
            ]
        return self.target.at[self.span(0, rows // 2, quarter), other * cols : (other + 1) * cols]


def weight_steps(weights, bounce, local_sem, send):
    z, r = lax.axis_index("dp"), lax.axis_index("row")
    count = len(weights)
    last = 3

    def keep_in(i):
        return pltpu.make_async_copy(weights[i].held(r, None), bounce[i], local_sem.at[i])

    def keep_out(i):
        return pltpu.make_async_copy(bounce[i], weights[i].whole(0, None), local_sem.at[i])

    over = []

    def start_over(i):
        if i < count:
            part = weights[i]
            over.append(send(part.held(1 - r, z), part.whole(1, z), {"row": 1 - r}))

    start_over(0)
    start_over(1)
    for i in range(count):
        keep_in(i).start()

    def hop(i, h, way):
        quarter = z - way * (h - 1)
        region = weights[i].whole(1, quarter)
        return region, {"dp": z + way}

    slots = {}
    for i in range(count):
        for h in (1, 2, 3):
            for way in (1, -1):
                slots[i, h, way] = send.slots
                send.slots += 1

    def copy(i, h, way):
        region, target = hop(i, h, way)
        slot = slots[i, h, way]
        return pltpu.make_async_remote_copy(
            src_ref=region,
            dst_ref=region,
            send_sem=send.send_sem.at[slot],
            recv_sem=send.recv_sem.at[slot],
            device_id=target,
            device_id_type=MESH,
        )

    def sends(h, way):
        if way > 0:
            return (z >= h - 1) & (z < last)
        return (z + h - 1 <= last) & (z > 0)

    def receives(h, way):
        return z >= h if way > 0 else z + h <= last

    def pass_on(i, h):
        for way in (1, -1):
            if h > 1:

                @pl.when(receives(h - 1, way))
                def _():
                    copy(i, h - 1, way).wait_recv()

            if h <= last:

                @pl.when(sends(h, way))
                def _():
                    copy(i, h, way).start()

    yield
    for i in range(count + 3):
        if i < count:
            over[i].wait_recv()
            start_over(i + 2)
            keep_in(i).wait()
            keep_out(i).start()
        for h in (1, 2, 3, 4):
            if 0 <= i - h + 1 < count:
                pass_on(i - h + 1, h)
        yield
    for i in range(count):
        keep_out(i).wait()
        for h in (1, 2, 3):
            for way in (1, -1):

                @pl.when(sends(h, way))
                def _():
                    copy(i, h, way).wait_send()


def scatter_steps(prepare, rows_part, rows_core, rows_x, rows_y, send, out_ref):
    half = rows_part.shape[1] // 2
    to_core, to_x, to_y = plane_peers()
    lo, hi = slice(0, half), slice(half, 2 * half)

    def summed(i, rows):
        return rows_part[4 + i, rows].astype(F32) + rows_core[i, rows].astype(F32)

    first = []
    for i in range(4):
        prepare(i)
        first.append(send(rows_part.at[i], rows_core.at[i], to_core))
    yield
    for i in range(4):
        prepare(4 + i)
    first[0].wait_recv()
    rows_part[4, lo] = summed(0, lo).astype(BF16)
    dx = send(rows_part.at[4, lo], rows_x.at[2], to_x)
    rows_part[4, hi] = summed(0, hi).astype(BF16)
    dy = send(rows_part.at[4, hi], rows_y.at[2], to_y)
    first[1].wait_recv()
    rows_part[5, lo] = summed(1, lo).astype(BF16)
    x0 = send(rows_part.at[5, lo], rows_x.at[0], to_x)
    first[2].wait_recv()
    rows_part[6, hi] = summed(2, hi).astype(BF16)
    y1 = send(rows_part.at[6, hi], rows_y.at[1], to_y)
    yield
    dy.wait_recv()
    rows_part[5, hi] = (summed(1, hi) + rows_y[2].astype(F32)).astype(BF16)
    x1 = send(rows_part.at[5, hi], rows_x.at[1], to_x)
    dx.wait_recv()
    rows_part[6, lo] = (summed(2, lo) + rows_x[2].astype(F32)).astype(BF16)
    y0 = send(rows_part.at[6, lo], rows_y.at[0], to_y)
    yield
    first[3].wait_recv()
    x0.wait_recv()
    y1.wait_recv()
    out_ref[lo] = summed(3, lo) + rows_x[0].astype(F32)
    out_ref[hi] = summed(3, hi) + rows_y[1].astype(F32)
    yield
    x1.wait_recv()
    out_ref[hi] = out_ref[hi] + rows_x[1].astype(F32)
    y0.wait_recv()
    out_ref[lo] = out_ref[lo] + rows_y[0].astype(F32)


SCATTERS = 10


def block_places():
    r, c, core, across = neighbours()
    ours = (4 + across, across, 4 + c, c)
    return [place + core - c for place in ours] + list(ours)


def scatter_rows(rows, width):
    half = rows // 2
    return [
        pltpu.VMEM((8, rows, width), BF16),
        pltpu.VMEM((4, rows, width), BF16),
        pltpu.VMEM((3, half, width), BF16),
        pltpu.VMEM((3, half, width), BF16),
    ]


def block_loads(part_ref, rows_part, sems):
    width = rows_part.shape[2]
    loads = []
    for i, place in enumerate(block_places()):
        cols = pl.ds(pl.multiple_of(place * width, width), width)
        loads.append(pltpu.make_async_copy(part_ref.at[:, cols], rows_part.at[i], sems.at[i]))
        loads[-1].start()
    return lambda i: loads[i].wait()


def dma(*counts):
    return [pltpu.SemaphoreType.DMA((count,)) for count in counts]


def gather_kernel(own_ref, out_ref, send_sem, recv_sem, local_sem):
    enter(plane_peers())
    send = Sender(send_sem, recv_sem)
    run(gather_steps(own_ref, out_ref, send, local_sem.at[0]))
    send.finish()


def gather_total_kernel(own_ref, vec_ref, out_ref, total_ref, got, send_sem, recv_sem, local_sem):
    enter(plane_peers())
    send = Sender(send_sem, recv_sem)
    run(
        total_steps(vec_ref, total_ref, got, send),
        gather_steps(own_ref, out_ref, send, local_sem.at[0]),
    )
    send.finish()


def scatter_kernel(part_ref, out_ref, *rest):
    rows, (send_sem, recv_sem, load_sem) = rest[:4], rest[4:]
    send = Sender(send_sem, recv_sem)
    prepare = block_loads(part_ref, rows[0], load_sem)
    enter(plane_peers())
    run(scatter_steps(prepare, *rows, send, out_ref))
    send.finish()


def scatter_total_kernel(part_ref, vec_ref, out_ref, total_ref, got, *rest):
    rows, (send_sem, recv_sem, load_sem) = rest[:4], rest[4:]
    send = Sender(send_sem, recv_sem)
    prepare = block_loads(part_ref, rows[0], load_sem)
    enter(plane_peers())
    run(
        total_steps(vec_ref, total_ref, got, send),
        scatter_steps(prepare, *rows, send, out_ref),
    )
    send.finish()


def start_kernel(
    own_ref,
    vec_ref,
    feed_ref,
    query,
    key,
    value,
    swish,
    output,
    wide,
    wide_feed,
    total,
    first_weight,
    out_weight,
    got,
    qk_bounce,
    vs_bounce,
    out_bounce,
    send_sem,
    recv_sem,
    local_sem,
):
    enter(plane_peers() + line_peers())
    send = Sender(send_sem, recv_sem)
    head, value_cols = query.shape[1] // 2, value.shape[1] // 2
    rows = query.shape[0]
    weights, bounce = [], []
    for i, (source, shift) in enumerate(((value, 2 * head), (swish, 2 * head + value_cols))):
        for part in range(2):
            weights.append(Weight(source, first_weight, "in", shift, part, 2))
            bounce.append(vs_bounce.at[i, part * rows // 2 : (part + 1) * rows // 2])
    for i, source in enumerate((query, key)):
        weights.append(Weight(source, first_weight, "in", i * head, 0, 1))
        bounce.append(qk_bounce.at[i])
    for part in range(2):
        weights.append(Weight(output, out_weight, "out", 0, part, 2))
        size = output.shape[0] // 4
        bounce.append(out_bounce.at[part * size : (part + 1) * size])
    run(
        weight_steps(weights, bounce, local_sem, send),
        total_steps(vec_ref, total, got, send),
        gather_timed(
            own_ref,
            wide,
            send,
            local_sem.at[8],
            {"x": 0, "x_here": 2, "y": 3, "y_here": 5, "diagonal": 8},
            True,
        ),
        gather_timed(
            feed_ref,
            wide_feed,
            send,
            local_sem.at[9],
            {"x": 2, "x_here": 4, "y": 5, "y_here": 8, "diagonal": 10},
            False,
        ),
    )
    send.finish()


def start(own, vector, feed, query, key, value, swish, output):
    rows, width = own.shape
    small = (rows // 128, 128)
    features, head, value_cols = 2 * query.shape[0], query.shape[1] // 2, value.shape[1] // 2
    wide = jax.ShapeDtypeStruct((rows, width * 8), BF16)
    count = 3 + 8 * 7 + 2 * GATHERS
    wide_one, wide_feed, total, first_weight, out_weight = pl.pallas_call(
        start_kernel,
        out_shape=(
            wide,
            wide,
            jax.ShapeDtypeStruct(small, F32),
            jax.ShapeDtypeStruct((features, 2 * head + 2 * value_cols), BF16),
            jax.ShapeDtypeStruct((output.shape[0] // 2, 2 * output.shape[1]), BF16),
        ),
        in_specs=vmem(3) + [anywhere()] * 5,
        out_specs=tuple(vmem(3) + [anywhere()] * 2),
        scratch_shapes=[
            pltpu.VMEM((5,) + small, F32),
            pltpu.VMEM((2, features // 2, head), BF16),
            pltpu.VMEM((2, features // 2, value_cols), BF16),
            pltpu.VMEM((output.shape[0] // 2, output.shape[1]), BF16),
        ]
        + dma(count, count, 10),
        compiler_params=params(5),
        name="start",
    )(own, vector.reshape(small), feed, query, key, value, swish, output)
    return wide_one, total.reshape(rows), wide_feed, first_weight, out_weight


def middle_scatter_kernel(part_ref, gelu, up, out_ref, second_weight, bounce, *rest):
    rows, (send_sem, recv_sem, load_sem, local_sem) = rest[:4], rest[4:]
    send = Sender(send_sem, recv_sem)
    prepare = block_loads(part_ref, rows[0], load_sem)
    enter(plane_peers() + line_peers())
    hidden_cols = gelu.shape[1] // 2
    weights, bounces = [], []
    for i, source in enumerate((gelu, up)):
        for part in range(2):
            weights.append(Weight(source, second_weight, "in", i * hidden_cols, part, 2))
            size = source.shape[0] // 2
            bounces.append(bounce.at[i, part * size : (part + 1) * size])
    run(
        weight_steps(weights, bounces, local_sem, send),
        scatter_steps(prepare, *rows, send, out_ref),
    )
    send.finish()


def middle_scatter(part, gelu, up):
    rows, wide = part.shape
    width, hidden_cols = wide // 8, gelu.shape[1] // 2
    count = SCATTERS + 4 * 7
    return pl.pallas_call(
        middle_scatter_kernel,
        out_shape=(
            jax.ShapeDtypeStruct((rows, width), F32),
            jax.ShapeDtypeStruct((2 * gelu.shape[0], 2 * hidden_cols), BF16),
        ),
        in_specs=[anywhere()] * 3,
        out_specs=tuple(vmem(1) + [anywhere()]),
        scratch_shapes=[pltpu.VMEM((2, gelu.shape[0], hidden_cols), BF16)]
        + scatter_rows(rows, width)
        + dma(count, count, 8, 4),
        compiler_params=params(6),
        name="middle_scatter",
    )(part, gelu, up)


def middle_gather_kernel(
    own_ref, vec_ref, down, out_ref, total_ref, last_weight, got, bounce, send_sem, recv_sem, local_sem
):
    enter(plane_peers() + line_peers())
    send = Sender(send_sem, recv_sem)
    size = down.shape[0] // 4
    run(
        weight_steps(
            [Weight(down, last_weight, "out", 0, part, 2) for part in range(2)],
            [bounce.at[part * size : (part + 1) * size] for part in range(2)],
            local_sem,
            send,
        ),
        total_steps(vec_ref, total_ref, got, send),
        gather_steps(own_ref, out_ref, send, local_sem.at[2]),
    )
    send.finish()


def middle_gather(own, vector, down):
    rows, width = own.shape
    small = (rows // 128, 128)
    count = 3 + GATHERS + 2 * 7
    wide, total, last_weight = pl.pallas_call(
        middle_gather_kernel,
        out_shape=(
            jax.ShapeDtypeStruct((rows, width * 8), own.dtype),
            jax.ShapeDtypeStruct(small, F32),
            jax.ShapeDtypeStruct((down.shape[0] // 2, 2 * down.shape[1]), BF16),
        ),
        in_specs=vmem(2) + [anywhere()],
        out_specs=tuple(vmem(2) + [anywhere()]),
        scratch_shapes=[
            pltpu.VMEM((5,) + small, F32),
            pltpu.VMEM((down.shape[0] // 2, down.shape[1]), BF16),
        ]
        + dma(count, count, 3),
        compiler_params=params(7),
        name="middle_gather",
    )(own, vector.reshape(small), down)
    return wide, total.reshape(rows), last_weight


def vmem(count):
    return [pl.BlockSpec(memory_space=VM)] * count


def anywhere():
    return pl.BlockSpec(memory_space=pl.ANY)


def params(number, limit=44):
    return pltpu.CompilerParams(
        collective_id=number, has_side_effects=True, vmem_limit_bytes=limit << 20
    )


def plane_gather(own):
    rows, width = own.shape
    return pl.pallas_call(
        gather_kernel,
        out_shape=jax.ShapeDtypeStruct((rows, width * 8), own.dtype),
        in_specs=vmem(1),
        out_specs=vmem(1)[0],
        scratch_shapes=dma(GATHERS, GATHERS, 1),
        compiler_params=params(0),
        name="gather",
    )(own)


def plane_gather_total(own, vector):
    rows, width = own.shape
    small = (rows // 128, 128)
    wide, total = pl.pallas_call(
        gather_total_kernel,
        out_shape=(
            jax.ShapeDtypeStruct((rows, width * 8), own.dtype),
            jax.ShapeDtypeStruct(small, F32),
        ),
        in_specs=vmem(2),
        out_specs=tuple(vmem(2)),
        scratch_shapes=[pltpu.VMEM((5,) + small, F32)] + dma(3 + GATHERS, 3 + GATHERS, 1),
        compiler_params=params(1),
    )(own, vector.reshape(small))
    return wide, total.reshape(rows)


def plane_scatter(part):
    rows, wide = part.shape
    width = wide // 8
    return pl.pallas_call(
        scatter_kernel,
        out_shape=jax.ShapeDtypeStruct((rows, width), F32),
        in_specs=[anywhere()],
        out_specs=vmem(1)[0],
        scratch_shapes=scatter_rows(rows, width) + dma(SCATTERS, SCATTERS, 8),
        compiler_params=params(2),
    )(part)


def plane_scatter_total(part, vector):
    rows, wide = part.shape
    width = wide // 8
    small = (rows // 128, 128)
    out, total = pl.pallas_call(
        scatter_total_kernel,
        out_shape=(jax.ShapeDtypeStruct((rows, width), F32), jax.ShapeDtypeStruct(small, F32)),
        in_specs=[anywhere()] + vmem(1),
        out_specs=tuple(vmem(2)),
        scratch_shapes=[pltpu.VMEM((5,) + small, F32)]
        + scatter_rows(rows, width)
        + dma(3 + SCATTERS, 3 + SCATTERS, 8),
        compiler_params=params(3),
        name="scatter",
    )(part, vector.reshape(small))
    return out, total.reshape(rows)


def swap_rows(values):
    return lax.ppermute(values, "row", [(0, 1), (1, 0)])


def halves_of(values, axis, r):
    size = values.shape[axis] // 2
    mine = lax.dynamic_slice_in_dim(values, r * size, size, axis)
    theirs = lax.dynamic_slice_in_dim(values, (1 - r) * size, size, axis)
    return mine, theirs


def whole_weight(values, axis, r):
    mine, theirs = halves_of(values, axis, r)
    return jnp.concatenate([mine, swap_rows(theirs)], axis=1 - axis)


PIECE = 128
GROUP = 8
OUT_UNITS = (0, 3)
UNITS = 7


def last_kernel(
    wide_one,
    wide_two,
    wide_att,
    wide_feed,
    gated,
    product,
    both_low,
    weight,
    feed_part,
    all_low,
    block_in,
    inner_vec,
    second_vec,
    result,
    back,
    feed,
    inner_out,
    gains,
    part,
    from_edge,
    from_inner,
    big,
    small,
    stream,
    rows_part,
    rows_core,
    rows_x,
    rows_y,
    total_got,
    gain_own,
    gain_got,
    load_sem,
    local_sem,
    free_sem,
    plane_send,
    plane_recv,
    gain_send,
    gain_recv,
    *line_sems,
):
    z, r, c = lax.axis_index("dp"), lax.axis_index("row"), lax.axis_index("col")
    barrier = pltpu.get_barrier_semaphore()
    peers = plane_peers() + line_peers()
    for target in peers:
        pl.semaphore_signal(barrier, inc=1, device_id=target, device_id_type=MESH)
    tokens, width = back.shape

    def load(slot, src, dst):
        return pltpu.make_async_copy(src, dst, load_sem.at[slot])

    hidden_cols = small.shape[2]
    loads = [
        load(0, wide_feed, big.at[0]),
        load(1, product, small.at[0]),
        load(2, wide_two, big.at[1]),
        load(3, both_low.at[:, hidden_cols:], small.at[1]),
        load(4, both_low.at[:, :hidden_cols], small.at[0]),
        load(5, wide_att, big.at[0]),
        load(6, gated, small.at[1]),
        load(7, wide_one, big.at[1]),
    ]
    for i in range(4):
        loads[i].start()

    places = block_places()
    feed_ready = block_loads(feed_part, rows_part, load_sem.at[10:18])

    def weight_load(i):
        rows = pl.ds(pl.multiple_of(places[i] * width, width), width)
        return load(8 + i % 2, weight.at[rows], stream.at[i % 2])

    weight_load(0).start()
    weight_load(1).start()
    pl.semaphore_wait(barrier, len(peers))

    is_edge = (z == 0) | (z == 3)
    is_inner = (z == 1) | (z == 2)
    near = jnp.where(z < 2, 1 - z, 5 - z)
    far = 3 - z
    flip = jnp.where((z == 0) | (z == 1), 1, 0)
    steps = UNITS * GROUP // 2

    def copy(stream_number, slot, src, dst, target):
        send_sem, recv_sem = line_sems[2 * stream_number], line_sems[2 * stream_number + 1]
        return pltpu.make_async_remote_copy(
            src_ref=src,
            dst_ref=dst,
            send_sem=send_sem.at[slot],
            recv_sem=recv_sem.at[slot],
            device_id=target,
            device_id_type=MESH,
        )

    def theirs_pair(q):
        return 2 * q + flip

    def mine_pair(q):
        return 2 * q + 1 - flip

    def final(pair, slot):
        unit, place = pair // GROUP, lax.rem(pair, GROUP)
        is_out = (unit == OUT_UNITS[0]) | (unit == OUT_UNITS[1])
        row = jnp.where(is_out, slot * 512 + (place // 2) * PIECE, place * PIECE)
        col = jnp.where(is_out, lax.rem(place, 2) * 512, slot * 512)
        return result.at[
            unit,
            pl.ds(pl.multiple_of(row, PIECE), PIECE),
            pl.ds(pl.multiple_of(col, 512), 512),
        ]

    def edge_copy(pair):
        return copy(0, pair, part.at[pair], from_edge.at[pair], {"dp": near})

    def inner_copy(q):
        return copy(1, q, part.at[theirs_pair(q)], from_inner.at[q], {"dp": far})

    def row_copy(q):
        pair = mine_pair(q)
        return copy(2, q, part.at[pair, 1 - r], final(pair, r), {"row": 1 - r})

    def row_arrival(q):
        pair = mine_pair(q)
        return copy(2, q, part.at[pair, 1 - r], final(pair, 1 - r), {"row": 1 - r})

    def keep_copy(q):
        pair = mine_pair(q)
        return pltpu.make_async_copy(part.at[pair, r], final(pair, r), local_sem.at[q])

    def own_copy(stream_number, q, pair, target):
        return copy(stream_number, q, part.at[pair, r], final(pair, r), {"dp": target})

    def got_copy(stream_number, q, pair, target):
        return copy(stream_number, q, final(pair, 1 - r), final(pair, 1 - r), {"dp": target})

    def pass_copy(slot, q, pair):
        return copy(7 + slot, q, final(pair, slot), final(pair, slot), {"dp": near})

    def compute(unit, x_ref, g_ref, shift=0):
        def body(j, carry):
            step, k = j // 2, lax.rem(j, 2)
            k = k + flip - 2 * k * flip
            place = 2 * step + k
            pair = unit * GROUP + place
            for slot in range(2):
                if unit in OUT_UNITS:
                    rows, cols = place // 2, lax.rem(place, 2) + 2 * slot
                else:
                    rows, cols = place + GROUP * slot, shift
                x = x_ref[:, pl.ds(pl.multiple_of(rows * PIECE, PIECE), PIECE)]
                g = g_ref[:, pl.ds(pl.multiple_of(cols * 512, 512), 512)]
                value = lax.dot_general(
                    x, g, (((0,), (0,)), ((), ())), preferred_element_type=F32
                )
                part[pair, r if slot == 0 else 1 - r] = value.astype(BF16)

            @pl.when(is_edge)
            def _():
                edge_copy(pair).start()

            return carry

        lax.fori_loop(0, GROUP, body, 0)

    def stage_far(q):
        pair = theirs_pair(q)
        edge_copy(pair).wait_recv()
        part[pair] = (part[pair].astype(F32) + from_edge[pair].astype(F32)).astype(BF16)
        inner_copy(q).start()

    def stage_sum(q):
        pair = mine_pair(q)
        edge_copy(pair).wait_recv()
        inner_copy(q).wait_recv()
        total = part[pair].astype(F32) + from_edge[pair].astype(F32) + from_inner[q].astype(F32)
        part[pair] = total.astype(BF16)
        row_copy(q).start()
        own_copy(3, q, pair, near).start()
        own_copy(4, q, pair, far).start()
        keep_copy(q).start()

    def stage_out(q):
        pair = mine_pair(q)
        row_arrival(q).wait_recv()
        got_copy(5, q, pair, near).start()
        got_copy(6, q, pair, far).start()

    def stage_pass(q):
        pair = theirs_pair(q)
        own_copy(4, q, pair, far).wait_recv()
        got_copy(6, q, pair, far).wait_recv()
        pass_copy(0, q, pair).start()
        pass_copy(1, q, pair).start()

    def step(q):
        for lag, stage in enumerate((stage_far, stage_sum, stage_out, stage_pass)):

            @pl.when((q >= lag) & (q < steps + lag))
            def _():
                stage(q - lag)

    def run_steps(first, last):
        @pl.when(is_inner)
        def _():
            lax.fori_loop(first, last, lambda q, carry: (step(q), carry)[1], 0)

    send = Sender(plane_send, plane_recv)

    def product_ready(i):
        weight_load(i).wait()

        def body(k, carry):
            rows = pl.ds(pl.multiple_of(k * 256, 256), 256)
            value = lax.dot_general(
                all_low[rows],
                stream[i % 2],
                (((1,), (1,)), ((), ())),
                preferred_element_type=F32,
            )
            rows_part[i, rows] = value.astype(BF16)
            return carry

        lax.fori_loop(0, tokens // 256, body, 0)
        if i < 6:
            weight_load(i + 2).start()

    def plane_steps():
        yield from scatter_steps(feed_ready, rows_part, rows_core, rows_x, rows_y, send, feed)
        send.finish()
        for target in plane_peers():
            pl.semaphore_signal(free_sem, inc=1, device_id=target, device_id_type=MESH)
        yield
        pl.semaphore_wait(free_sem, 3)
        beside = total_steps(inner_vec, inner_out, total_got, send)
        for _ in scatter_steps(product_ready, rows_part, rows_core, rows_x, rows_y, send, back):
            next(beside, None)
            yield
        first_gain = jnp.sum(back[...] * block_in[...].astype(F32), axis=0, keepdims=True)
        gain_own[0:1] = first_gain
        gain_own[1:2] = second_vec[...]
        for each in gain_copies:
            each.start()
        yield
        send.finish()

    gain_copies = [
        pltpu.make_async_remote_copy(
            src_ref=gain_own,
            dst_ref=gain_got.at[k - 1],
            send_sem=gain_send.at[k - 1],
            recv_sem=gain_recv.at[k - 1],
            device_id={"dp": lax.rem(z + k, 4)},
            device_id_type=MESH,
        )
        for k in (1, 2, 3)
    ]

    loads[0].wait()
    loads[1].wait()
    compute(0, small.at[0], big.at[0])
    loads[4].start()
    loads[5].start()
    plane = plane_steps()
    done = 0
    later = {
        4: (1, (2, 3), lambda: (big.at[1], small.at[1]), (6,)),
        8: (2, (4,), lambda: (big.at[1], small.at[0]), (7,)),
        12: (3, (5, 6), lambda: (small.at[1], big.at[0]), ()),
        16: (4, (7,), lambda: (big.at[1], all_low, 0), ()),
        20: (5, (), lambda: (big.at[1], all_low, 1), ()),
        24: (6, (), lambda: (big.at[1], all_low, 2), ()),
    }
    while done < 28:
        next(plane, None)
        run_steps(done, done + 1)
        done += 1
        if done + 1 in later:
            unit, before, arguments, after = later[done + 1]
            for i in before:
                loads[i].wait()
            compute(unit, *arguments())
            for i in after:
                loads[i].start()
    for _ in plane:
        pass
    run_steps(done, steps + 3)

    total = gain_own[...]
    for each in gain_copies:
        each.wait_send()
    for k in range(3):
        gain_copies[k].wait_recv()
        total = total + gain_got[k]
    gains[...] = total

    @pl.when(is_inner)
    def _():
        def body(q, carry):
            pair = mine_pair(q)
            inner_copy(q).wait_send()
            row_copy(q).wait_send()
            own_copy(3, q, pair, near).wait_send()
            own_copy(4, q, pair, far).wait_send()
            got_copy(5, q, pair, near).wait_send()
            got_copy(6, q, pair, far).wait_send()
            keep_copy(q).wait()
            for slot in range(2):
                pass_copy(slot, q, theirs_pair(q)).wait_send()
            return carry

        lax.fori_loop(0, steps, body, 0)

    @pl.when(is_edge)
    def _():
        def body(q, carry):
            edge_copy(theirs_pair(q)).wait_send()
            edge_copy(mine_pair(q)).wait_send()
            own_copy(3, q, mine_pair(q), near).wait_recv()
            got_copy(5, q, mine_pair(q), near).wait_recv()
            for slot in range(2):
                pass_copy(slot, q, theirs_pair(q)).wait_recv()
            return carry

        lax.fori_loop(0, steps, body, 0)


def last_scatter(
    wide_one,
    wide_two,
    wide_att,
    wide_feed,
    gated,
    product,
    both_low,
    weight,
    feed_part,
    all_low,
    own,
    inner,
    second,
):
    tokens, width = own.shape
    small = (tokens // 128, 128)
    pairs = UNITS * GROUP
    steps = pairs // 2
    shape = (pairs, 2, PIECE, 512)
    gain_shape = (8, width)
    scratch = [
        pltpu.VMEM(shape, BF16),
        pltpu.VMEM(shape, BF16),
        pltpu.VMEM((steps,) + shape[1:], BF16),
        pltpu.VMEM((2,) + wide_one.shape, BF16),
        pltpu.VMEM((2,) + gated.shape, BF16),
        pltpu.VMEM((2, width, weight.shape[1]), BF16),
        *scatter_rows(tokens, width),
        pltpu.VMEM((5,) + small, F32),
        pltpu.VMEM(gain_shape, F32),
        pltpu.VMEM((3,) + gain_shape, F32),
        *dma(18, steps),
        pltpu.SemaphoreType.REGULAR,
        *dma(2 * SCATTERS + 3, 2 * SCATTERS + 3, 3, 3),
    ]
    for size in (pairs,) + (steps,) * 8:
        scratch += dma(size, size)
    result, back, feed, total, gains = pl.pallas_call(
        last_kernel,
        out_shape=(
            jax.ShapeDtypeStruct((UNITS, 1024, 1024), BF16),
            jax.ShapeDtypeStruct((tokens, width), F32),
            jax.ShapeDtypeStruct((tokens, width), F32),
            jax.ShapeDtypeStruct(small, F32),
            jax.ShapeDtypeStruct(gain_shape, F32),
        ),
        in_specs=[anywhere()] * 9 + vmem(4),
        out_specs=tuple([anywhere()] + vmem(4)),
        scratch_shapes=scratch,
        compiler_params=params(4, 62),
        name="last_scatter",
    )(
        wide_one,
        wide_two,
        wide_att,
        wide_feed,
        gated,
        product,
        both_low,
        weight,
        feed_part,
        all_low,
        own,
        inner.reshape(small),
        second.reshape(1, width),
    )
    return result, back, feed, total.reshape(tokens), gains[0], gains[1]


def place_halves(mine, theirs, axis, r):
    both = jnp.concatenate([mine, theirs, mine], axis=axis)
    width = mine.shape[axis]
    return lax.dynamic_slice_in_dim(both, r * width, 2 * width, axis).astype(F32)


def sum_packs(grads):
    r = lax.axis_index("row")
    totals = lax.psum(tuple(grad for grad, axis in grads), "dp")
    placed = []
    for total, (grad, axis) in zip(totals, grads):
        size = total.shape[1 - axis] // 2
        mine = lax.slice_in_dim(total, 0, size, axis=1 - axis)
        theirs = swap_rows(lax.slice_in_dim(total, size, 2 * size, axis=1 - axis))
        placed.append(place_halves(mine, theirs, axis, r))
    return placed


def matmul(left, right):
    return jnp.dot(left, right, preferred_element_type=jnp.float32)


def weight_grad(inputs, grads):
    return jnp.einsum("tk,tf->kf", inputs, grads, preferred_element_type=jnp.float32).astype(BF16)


def back_product(grads, weights):
    return jnp.einsum("tf,kf->tk", grads, weights, preferred_element_type=jnp.float32)


def group_norm(retained):
    spread = jnp.sqrt(jnp.mean(retained * retained, axis=1, keepdims=True) + epsilon)
    return retained / jnp.maximum(spread, 1.0)


def swish_gate(swish_sum, grouped):
    return jax.nn.silu(swish_sum) * grouped


def gelu_gate(gelu_sum, up_sum):
    return jax.nn.gelu(gelu_sum) * up_sum


def retention(query_low, key_low, value_low, segments, log_decay):
    outputs = []
    for start in range(0, query_low.shape[0], QBLK):
        stop = start + QBLK
        decay = decay_block(segments, start, QBLK, stop, log_decay)
        scores = jnp.einsum(
            "qd,kd->qk", query_low[start:stop], key_low[:stop], preferred_element_type=jnp.float32
        )
        weights_low = (scores * decay).astype(jnp.bfloat16)
        outputs.append(matmul(weights_low, value_low[:stop]))
    return jnp.concatenate(outputs, axis=0)


def retention_back(query_low, key_low, value_low, retained_low, segments, log_decay):
    tokens = query_low.shape[0]
    key_accum = jnp.zeros((tokens, key_low.shape[1]), jnp.float32)
    value_accum = jnp.zeros((tokens, value_low.shape[1]), jnp.float32)
    query_parts = []
    for start in range(0, tokens, QBLK):
        stop = start + QBLK
        decay = decay_block(segments, start, QBLK, stop, log_decay)
        scores = jnp.einsum(
            "qd,kd->qk", query_low[start:stop], key_low[:stop], preferred_element_type=jnp.float32
        )
        weights_low = (scores * decay).astype(jnp.bfloat16)
        weights_grad = jnp.einsum(
            "qv,kv->qk",
            retained_low[start:stop],
            value_low[:stop],
            preferred_element_type=jnp.float32,
        )
        scores_low = (weights_grad * decay).astype(jnp.bfloat16)
        query_parts.append(matmul(scores_low, key_low[:stop]))
        key_accum = key_accum.at[:stop].add(
            jnp.einsum(
                "qk,qd->kd", scores_low, query_low[start:stop], preferred_element_type=jnp.float32
            )
        )
        value_accum = value_accum.at[:stop].add(
            jnp.einsum(
                "qk,qv->kv",
                weights_low,
                retained_low[start:stop],
                preferred_element_type=jnp.float32,
            )
        )
    return jnp.concatenate(query_parts, axis=0), key_accum, value_accum


def shards(
    block_in,
    segment_ids,
    block_cotangent,
    query_weight,
    key_weight,
    value_weight,
    swish_weight,
    output_weight,
    gelu_weight,
    up_weight,
    down_weight,
    first_gain,
    second_gain,
):
    r = lax.axis_index("row")
    hidden = block_in[0].astype(jnp.float32)
    segments = segment_ids[0]
    tokens = hidden.shape[0]
    features = hidden.shape[1] * lax.axis_size("row") * lax.axis_size("col")
    head_index = lax.axis_index("col") * lax.axis_size("row") + r
    log_decay = jnp.log(1.0 - 2.0 ** (-5.0 - head_index.astype(jnp.float32)))
    cosine_table, sine_table = rotary_tables(tokens, KD)

    value_cols = value_weight.shape[1] // 2
    hidden_cols = gelu_weight.shape[1] // 2
    line = lax.axis_size("dp") == 4
    if not line:
        first_weight = jnp.concatenate(
            [
                whole_weight(weight, 1, r)
                for weight in (query_weight, key_weight, value_weight, swish_weight)
            ],
            axis=1,
        )
        out_weight = whole_weight(output_weight, 0, r)
        second_weight = jnp.concatenate(
            [whole_weight(gelu_weight, 1, r), whole_weight(up_weight, 1, r)], axis=1
        )
        last_weight = whole_weight(down_weight, 0, r)

    own_one, own_square = (hidden * first_gain).astype(BF16), jnp.sum(hidden * hidden, axis=1)
    if line:
        wide_one, square_one, wide_feed_grad, first_weight, out_weight = start(
            own_one,
            own_square,
            block_cotangent[0],
            query_weight,
            key_weight,
            value_weight,
            swish_weight,
            output_weight,
        )
    else:
        wide_one, square_one = plane_gather_total(own_one, own_square)
        wide_feed_grad = plane_gather(block_cotangent[0])
    scale_one = lax.rsqrt(square_one / features + epsilon)[:, None]
    sums_one = matmul(wide_one, first_weight) * scale_one
    query_sum = sums_one[:, :KD]
    key_sum = sums_one[:, KD : 2 * KD]
    value_sum = sums_one[:, 2 * KD : 2 * KD + value_cols]
    swish_sum = sums_one[:, 2 * KD + value_cols :]
    query_low = (query_sum * cosine_table + rotate_half(query_sum) * sine_table).astype(
        jnp.bfloat16
    )
    key_low = ((key_sum * cosine_table + rotate_half(key_sum) * sine_table) * KD ** (-0.5)).astype(
        jnp.bfloat16
    )
    value_low = value_sum.astype(jnp.bfloat16)
    retained = retention(query_low, key_low, value_low, segments, log_decay)
    grouped, group_pull = jax.vjp(group_norm, retained)
    gated_full, swish_pull = jax.vjp(swish_gate, swish_sum, grouped)
    gated = gated_full.astype(jnp.bfloat16)
    attended = matmul(gated, out_weight).astype(BF16)
    if line:
        attended, second_weight = middle_scatter(attended, gelu_weight, up_weight)
    else:
        attended = plane_scatter(attended)
    middle = hidden + attended

    own_two, own_square = (middle * second_gain).astype(BF16), jnp.sum(middle * middle, axis=1)
    if line:
        wide_two, square_two, last_weight = middle_gather(own_two, own_square, down_weight)
    else:
        wide_two, square_two = plane_gather_total(own_two, own_square)
    scale_two = lax.rsqrt(square_two / features + epsilon)[:, None]
    sums_two = matmul(wide_two, second_weight) * scale_two
    gelu_sum, up_sum = sums_two[:, :hidden_cols], sums_two[:, hidden_cols:]
    product_full, gelu_pull = jax.vjp(gelu_gate, gelu_sum, up_sum)
    product = product_full.astype(jnp.bfloat16)
    feed_part = matmul(product, last_weight).astype(BF16)

    upstream = block_cotangent[0].astype(jnp.float32)
    product_grad = back_product(wide_feed_grad, last_weight)
    gelu_grad, up_grad = gelu_pull(product_grad)
    both_grad = jnp.concatenate([gelu_grad, up_grad], axis=1)
    inner_two = jnp.sum(both_grad * sums_two, axis=1)
    both_low = (both_grad * scale_two).astype(BF16)
    normed_two_grad, inner_two = plane_scatter_total(
        back_product(both_low, second_weight).astype(BF16), inner_two
    )
    middle_grad = (
        upstream
        + second_gain * normed_two_grad
        - middle * (scale_two**2 * inner_two[:, None] / features)
    )
    wide_attended_grad = plane_gather(middle_grad.astype(BF16))
    gated_grad = back_product(wide_attended_grad, out_weight)
    swish_grad, grouped_grad = swish_pull(gated_grad)
    (retained_grad,) = group_pull(grouped_grad)
    query_grad, key_grad, value_grad = retention_back(
        query_low, key_low, value_low, retained_grad.astype(BF16), segments, log_decay
    )
    key_grad = key_grad * KD ** (-0.5)
    query_back = query_grad * cosine_table - rotate_half(query_grad) * sine_table
    key_back = key_grad * cosine_table - rotate_half(key_grad) * sine_table
    all_grad = jnp.concatenate([query_back, key_back, value_grad, swish_grad], axis=1)
    inner_one = jnp.sum(all_grad * sums_one, axis=1)
    all_low = (all_grad * scale_one).astype(BF16)
    own_second = jnp.sum(normed_two_grad * middle, axis=0)
    if line:
        result, normed_one_grad, feed, inner_one, grad_first, grad_second = last_scatter(
            wide_one,
            wide_two,
            wide_attended_grad,
            wide_feed_grad,
            gated,
            product,
            both_low,
            first_weight,
            feed_part,
            all_low,
            block_in[0],
            inner_one,
            own_second,
        )
        grad_down, grad_up, grad_gelu, grad_output = [result[i].astype(F32) for i in range(4)]
        starts = (0, 2 * KD)
        grad_query, grad_key = [
            jnp.concatenate(
                [result[4, :, side + shift : side + shift + KD] for side in starts], axis=1
            ).astype(F32)
            for shift in (0, KD)
        ]
        grad_value, grad_swish = result[5].astype(F32), result[6].astype(F32)
    else:
        feed = plane_scatter(feed_part)
        normed_one_grad, inner_one = plane_scatter_total(
            back_product(all_low, first_weight).astype(BF16), inner_one
        )
        grad_first, grad_second = lax.psum(
            (jnp.sum(normed_one_grad * hidden, axis=0), own_second), "dp"
        )
        grad_all = weight_grad(wide_one, all_low)
        (
            grad_query,
            grad_key,
            grad_value,
            grad_swish,
            grad_output,
            grad_gelu,
            grad_up,
            grad_down,
        ) = sum_packs(
            (
                (grad_all[:, :KD], 1),
                (grad_all[:, KD : 2 * KD], 1),
                (grad_all[:, 2 * KD : 2 * KD + value_cols], 1),
                (grad_all[:, 2 * KD + value_cols :], 1),
                (weight_grad(gated, wide_attended_grad), 0),
                (weight_grad(wide_two, both_low[:, :hidden_cols]), 1),
                (weight_grad(wide_two, both_low[:, hidden_cols:]), 1),
                (weight_grad(product, wide_feed_grad), 0),
            )
        )
    block_out = (middle + feed).astype(BF16)
    grad_input = (
        middle_grad
        + first_gain * normed_one_grad
        - hidden * (scale_one**2 * inner_one[:, None] / features)
    ).astype(BF16)

    return (
        block_out[None],
        grad_input[None],
        grad_query,
        grad_key,
        grad_value,
        grad_swish,
        grad_output,
        grad_gelu,
        grad_up,
        grad_down,
        grad_first,
        grad_second,
    )


def solution(mesh):
    activations = P("dp", None, ("row", "col"))
    in_weight, out_weight, gain = P("row", "col"), P("col", "row"), P(("row", "col"))
    return jax.shard_map(
        shards,
        mesh=mesh,
        in_specs=(activations, P("dp", None), activations)
        + (in_weight,) * 4
        + (out_weight, in_weight, in_weight, out_weight, gain, gain),
        out_specs=(activations, activations)
        + (in_weight,) * 4
        + (out_weight, in_weight, in_weight, out_weight, gain, gain),
        check_vma=False,
    )
```
